32 devices in a mesh: tm: 4 (over y, x), lat: 4 (over z), ens: 2 (over core).
Axes of the slice: x: 2, y: 2, z: 4, core: 2. Of those that a mesh axis runs over, the one named last changes fastest.
Arguments:
- increment: float32 [4, 4, 64, 1440], P('tm', None, 'lat'), may hold values from -6 to 6
- wind_lon: float32 [4, 4, 64, 1440], P('tm', None, 'lat'), may hold values from -0.45 to 0.45
- wind_lat: float32 [4, 4, 64, 1440], P('tm', None, 'lat'), may hold values from -0.45 to 0.45
- model_precision: float32 [4], replicated, may hold values from 0.5 to 4
- perturbations: float32 [32, 4, 64, 1440], P('ens', 'tm', 'lat'), may hold values from -0.24350093 to 0.24350093
- obs_rows: int32 [4, 128], P('tm', 'lat'), may hold values from 0 to 63
- obs_jacobian: float32 [4, 128, 16, 1440], P('tm', 'lat'), may hold values from -0.15625 to 0.15625
- obs_values: float32 [4, 128, 16], P('tm', 'lat'), may hold values from -6 to 6
- obs_precision: float32 [4, 128, 16], P('tm', 'lat'), may hold values from 0.5 to 2
- obs_counts: int32 [4, 128], P('tm', 'lat'), may hold values from 1 to 16
Outputs:
- grad_state: float32 [4, 4, 64, 1440], P('tm', None, 'lat')
- forcing_step: float32 [4, 64, 1440], P('tm', 'lat')
The draws below stay inside these ranges and needn't reach their ends.
Inputs may be any that keep to these rules, and one draw needn't show every extreme that they name: `obs_rows`: block j of band b reads level r // 16 and latitude b * 16 + r % 16, where r is its entry; several blocks may read the same row. `obs_counts`: only the first count slots of a block hold observations.
All inputs are finite; a program needn't handle non-finite values.
Results may differ from the reference program's by a relative error of at most 0.0003.
Values sent between devices are 32-bit elements; how exact they have to be, the bound alone decides.
A program may use at most 64 MiB of HBM per device.

```python
import math
import jax
import jax.numpy as jnp
from jax import lax

NLON = 1440
MEM = 32
CLAT = 16
STEPS = 4
OBS = 32
NOB = 16
NT = 4
LEV = 4
NLAT = 64
OBSALL = 128


def with_ends(entries, rng, least, top_value):
    longest = entries.shape.index(max(entries.shape))
    spots = []
    for shift in (0, 1):
        where = [jax.random.randint(jax.random.fold_in(rng, axis), (), 0, length) for axis, length in enumerate(entries.shape)]
        where[longest] = (where[longest] + shift) % entries.shape[longest]
        spots.append(tuple(where))
    return entries.at[spots[0]].set(least).at[spots[1]].set(top_value)


def shard_levels(own_key, extent, split, least, top_value):
    level = 1.0
    for axis_at, shards_of in split:
        draws = jax.random.uniform(jax.random.fold_in(jax.random.fold_in(own_key, 6), axis_at), (shards_of,), jnp.float32, least / len(split), top_value / len(split))
        level = level * jnp.repeat(jnp.exp(draws), extent[axis_at] // shards_of).reshape((-1,) + (1,) * (len(extent) - 1 - axis_at))
    return level


def noise(rng, extent, spread, most, pieces=(), kind=jnp.bfloat16):
    loudness = shard_levels(rng, extent, pieces, -0.22, 0.18) if pieces else 1.0
    entries = jax.random.normal(rng, extent, jnp.float32) * spread * loudness
    return jnp.minimum(jnp.maximum(entries, -most), most).astype(kind)


def setup_inputs(seed: int = 0) -> dict:
    arg_keys = jax.random.split(jax.random.key(seed), 11)
    return {
        "increment": noise(arg_keys[0], (NT, LEV, NLAT, NLON), 1.0, 6.0, ((0, 4), (2, 4)), jnp.float32),
        "wind_lon": jnp.clip(jax.random.uniform(arg_keys[1], (NT, LEV, NLAT, NLON), jnp.float32, -0.45, 0.45) * shard_levels(arg_keys[1], (NT, LEV, NLAT, NLON), ((0, 4), (2, 4)), -0.4, 0.0), -0.45, 0.45),
        "wind_lat": jnp.clip(jax.random.uniform(arg_keys[2], (NT, LEV, NLAT, NLON), jnp.float32, -0.45, 0.45) * shard_levels(arg_keys[2], (NT, LEV, NLAT, NLON), ((0, 4), (2, 4)), -0.4, 0.0), -0.45, 0.45),
        "model_precision": jnp.clip(jnp.exp(jax.random.uniform(arg_keys[3], (LEV,), jnp.float32, math.log(0.5), math.log(4.0))), 0.5, 4.0),
        "perturbations": noise(arg_keys[4], (MEM, LEV, NLAT, NLON), ((LEV * NLAT * NLON) ** -0.25), 0.24350093, ((0, 2), (1, 4), (2, 4)), jnp.float32),
        "obs_rows": with_ends(jax.random.randint(arg_keys[5], (NT, OBSALL), 0, LEV * CLAT), jax.random.fold_in(arg_keys[5], 1), 0, (LEV * CLAT) - 1).astype(jnp.int32),
        "obs_jacobian": noise(arg_keys[6], (NT, OBSALL, NOB, NLON), NLON ** -0.5, 0.15625, ((0, 4), (1, 4)), jnp.float32),
        "obs_values": noise(arg_keys[7], (NT, OBSALL, NOB), 1.0, 6.0, ((0, 4), (1, 4)), jnp.float32),
        "obs_precision": jnp.clip(jnp.exp(math.log(2.0) - 1.3862944 * jax.random.uniform(arg_keys[8], (NT, OBSALL, NOB), jnp.float32) ** shard_levels(arg_keys[8], (NT, OBSALL, NOB), ((0, 4), (1, 4)), -0.2, 0.2)), 0.5, 2.0),
        "obs_counts": with_ends(jax.random.randint(arg_keys[9], (NT, OBSALL), 1, NOB + 1), jax.random.fold_in(arg_keys[9], 1), 1, NOB).astype(jnp.int32),
    }


def coefficients(wind_lon, wind_lat):
    center = 1.0 - wind_lon * wind_lon - wind_lat * wind_lat
    plus_lon = 0.5 * (wind_lon * wind_lon - wind_lon)
    minus_lon = 0.5 * (wind_lon * wind_lon + wind_lon)
    plus_lat = 0.5 * (wind_lat * wind_lat - wind_lat)
    minus_lat = 0.5 * (wind_lat * wind_lat + wind_lat)
    return (center, plus_lon, minus_lon, plus_lat, minus_lat)


def advect(field, coefs):
    center, plus_lon, minus_lon, plus_lat, minus_lat = coefs
    northern = jnp.pad(field[:, 1:], ((0, 0), (0, 1), (0, 0)))
    southern = jnp.pad(field[:, :-1], ((0, 0), (1, 0), (0, 0)))
    return (center * field + plus_lon * jnp.roll(field, -1, 2) + minus_lon * jnp.roll(field, 1, 2)
            + plus_lat * northern + minus_lat * southern)


def advect_adjoint(field, coefs):
    center, plus_lon, minus_lon, plus_lat, minus_lat = coefs
    upward = plus_lat * field
    downward = minus_lat * field
    from_south = jnp.pad(upward[:, :-1], ((0, 0), (1, 0), (0, 0)))
    from_north = jnp.pad(downward[:, 1:], ((0, 0), (0, 1), (0, 0)))
    return (center * field + jnp.roll(plus_lon * field, 1, 2) + jnp.roll(minus_lon * field, -1, 2)
            + from_south + from_north)


def reference(increment, wind_lon, wind_lat, model_precision, perturbations, obs_rows, obs_jacobian,
              obs_values, obs_precision, obs_counts):
    highest = lax.Precision.HIGHEST
    level_prec = model_precision[:, None, None]
    band = jnp.arange(OBSALL, dtype=jnp.int32) // OBS
    slots = jnp.arange(NOB, dtype=jnp.int32)
    ends = []
    coef_list = []
    for window in range(NT):
        coefs = coefficients(wind_lon[window], wind_lat[window])
        coef_list.append(coefs)
        field = increment[window]
        for repeat in range(STEPS):
            field = advect(field, coefs)
        ends.append(field)
    mismatches = []
    for window in range(NT):
        if window > 0:
            mismatches.append(level_prec * (increment[window] - ends[window - 1]))
        else:
            mismatches.append(level_prec * increment[window])
    grads = []
    total = jnp.zeros((LEV, NLAT, NLON), jnp.float32)
    for window in range(NT):
        coefs = coef_list[window]
        rows = obs_rows[window].astype(jnp.int32)
        level = rows // CLAT
        latitude = band * CLAT + rows % CLAT
        picked = ends[window][level, latitude]
        jacobian = obs_jacobian[window]
        evolved = jnp.einsum('jon,jn->jo', jacobian, picked, precision=highest)
        used = (slots[None, :] < obs_counts[window][:, None]).astype(jnp.float32)
        weighted = obs_precision[window] * (evolved - obs_values[window]) * used
        force = jnp.einsum('jon,jo->jn', jacobian, weighted, precision=highest)
        adjoint = jnp.zeros((LEV, NLAT, NLON), jnp.float32).at[level, latitude].add(force)
        if window + 1 < NT:
            adjoint = adjoint - mismatches[window + 1]
        forcing = adjoint
        for repeat in range(STEPS):
            adjoint = advect_adjoint(adjoint, coefs)
            if repeat + 1 < STEPS:
                forcing = forcing + adjoint
        grads.append(adjoint + mismatches[window])
        total = total + forcing
    member_coef = jnp.einsum('mlan,lan->m', perturbations, total, precision=highest)
    forcing_step = -jnp.einsum('m,mlan->lan', member_coef, perturbations, precision=highest) / (MEM - 1.0)
    return jnp.stack(grads), forcing_step
```

```python
import functools

import jax
import jax.numpy as jnp
from jax import lax
from jax.experimental import pallas as pl
from jax.experimental.pallas import tpu as pltpu
from jax.sharding import PartitionSpec as P

STEPS = 4
MESH = pl.DeviceIdType.MESH
HIGHEST = lax.Precision.HIGHEST
NN = (((1,), (0,)), ((), ()))


def mm(a, b, dims, precision=None):
    return lax.dot_general(a, b, dims, precision=precision, preferred_element_type=jnp.float32)


def split(value):
    hi = value.astype(jnp.bfloat16)
    lo = (value - hi.astype(jnp.float32)).astype(jnp.bfloat16)
    return hi, lo


def turn(value, steps, axis):
    return pltpu.roll(value, steps % value.shape[axis], axis)


def extend(ref, where, lon):
    width = ref.shape[-1]
    rem = lon % 128
    last = ref[where + (slice(0, 16), slice(width - 128, width))]
    before = ref[where + (slice(0, 16), slice(width - 256, width - 128))]
    first = ref[where + (slice(0, 16), slice(0, 128))]
    lane = lax.broadcasted_iota(jnp.int32, last.shape, 1)
    wrapped = jnp.where(lane < 128 - rem, turn(before, 128 - rem, 1), turn(last, 128 - rem, 1))
    right = jnp.where(lane < rem + (128 - rem) // 2, turn(first, rem, 1), wrapped)
    ref[where + (slice(0, 16), slice(width - 128, width))] = jnp.where(lane < rem, last, right)


def kernel(
    T, L, E,
    rows_hbm, cnt_hbm, val_hbm, prc_hbm, mp_hbm, inc_hbm, wlon_hbm, wlat_hbm, jac_hbm, pert_hbm,
    grad_v, pert_v, cb_v,
    rows_s, rows_ref, cnt_ref, val_ref, prc_ref, mp_ref, fields, jac_v, tail, val_b, prc_b, part_v, wgt, pick,
    wide, coef, adj, h_first, h_last, h_after, h_before, a_up_v, a_down_v, a_after, a_before,
    end_v, lines, nxt_v, prior_v, forc, edge, rs_v, edge_v, ca_send, ca_v, cb_send,
    load_sem, small_sem, h_ssem, h_rsem, a_ssem, a_rsem, t_ssem, t_rsem, e_ssem, e_rsem, p_ssem, p_rsem,
    rs_ssem, rs_rsem, ed_ssem, ed_rsem, ca_ssem, ca_rsem, cb_ssem, cb_rsem, g_ssem, g_rsem, all_sem,
):
    k, b, e = lax.axis_index("tm"), lax.axis_index("lat"), lax.axis_index("ens")
    _, half, crow, lon = fields.shape
    width = wide.shape[-1]
    members = pert_v.shape[1]
    slots, blocks = val_ref.shape
    tiles, rem = width // 128, lon % 128
    other = 1 - e
    own = pl.ds(e * half, half)

    def shift(at):
        return lax.rem(at + at // 2 + 1 + e, half)

    def spot(t, at, there):
        return lax.rem(t + shift(at) + half - shift(there), half)

    order = [lax.rem(shift(k) + t, half) for t in range(half)]
    level = [e * half + at for at in order]

    def local(src, dst, sem):
        return pltpu.make_async_copy(src, dst, sem)

    for at, ref in enumerate((inc_hbm, wlon_hbm, wlat_hbm)):
        for t in range(half):
            local(ref.at[level[t]], fields.at[at, t], load_sem.at[0]).start()
    small = [
        local(rows_hbm, rows_s, small_sem.at[0]),
        local(rows_hbm, rows_ref, small_sem.at[1]),
        local(cnt_hbm, cnt_ref, small_sem.at[2]),
        local(val_hbm, val_ref, small_sem.at[3]),
        local(prc_hbm, prc_ref, small_sem.at[4]),
        local(mp_hbm, mp_ref, small_sem.at[5]),
    ]

    barrier = pltpu.get_barrier_semaphore()
    direct = T * L * E <= 64
    group = [(dt, de) for dt in range(T) for de in range(E) if dt or de]

    def mate(dt, de):
        return {"tm": lax.rem(k + dt, T), "ens": lax.rem(e + de, E)}

    for dt, de in group:
        pl.semaphore_signal(barrier, inc=1, device_id=mate(dt, de), device_id_type=MESH)
    for db in range(1, L):
        pl.semaphore_signal(barrier, inc=1, device_id={"lat": lax.rem(b + db, L)}, device_id_type=MESH)

    def remote(src, dst, ssem, rsem, device):
        return pltpu.make_async_remote_copy(
            src_ref=src, dst_ref=dst, send_sem=ssem, recv_sem=rsem, device_id=device, device_id_type=MESH
        )

    up = {"lat": lax.rem(b + 1, L)}
    down = {"lat": lax.rem(b + L - 1, L)}
    later_k, prior_k = lax.rem(k + 1, T), lax.rem(k + T - 1, T)
    partner = {"ens": other}
    has_up, has_down = b < L - 1, b > 0
    has_later, has_prior = k < T - 1, k > 0

    local(fields, fields, load_sem.at[0]).wait()
    jac_load = local(jac_hbm, jac_v, load_sem.at[1])
    pert_load = local(pert_hbm, pert_v.at[e], load_sem.at[2])
    for item in small + [pert_load, jac_load]:
        item.start()
    for t in range(half):
        for at in range(3):
            wide[at, t, 0:16, 0:lon] = fields[at, t]
            extend(wide, (at, t), lon)
        h_first[t, 0] = wide[0, t, 0:2]
        h_first[t, 1] = wide[0, t, 2:4]
        h_last[t, 0] = wide[0, t, crow - 4 : crow - 2]
        h_last[t, 1] = wide[0, t, crow - 2 : crow]
        for at in (1, 2):
            h_first[t, 1 + at] = wide[at, t, 0:2]
            h_first[t, 4, at - 1 : at] = wide[at, t, 2:3]
            h_last[t, 1 + at] = wide[at, t, crow - 2 : crow]
            h_last[t, 4, at - 1 : at] = wide[at, t, crow - 3 : crow - 2]

    pl.semaphore_wait(barrier, len(group) + L - 1)
    if direct:
        for db in range(1, L):
            pl.semaphore_signal(all_sem, inc=1, device_id={"lat": lax.rem(b + db, L)}, device_id_type=MESH)

    h_up = [remote(h_last.at[t], h_before.at[t], h_ssem.at[0], h_rsem.at[0, t], up) for t in range(half)]
    h_down = [remote(h_first.at[t], h_after.at[t], h_ssem.at[1], h_rsem.at[1, t], down) for t in range(half)]
    n_copy = [
        remote(fields.at[0, spot(t, prior_k, k)], nxt_v.at[t], t_ssem, t_rsem.at[t], {"tm": prior_k})
        for t in range(half)
    ]

    def e_copy(t):
        there = spot(t, k, later_k)
        return remote(end_v.at[t], prior_v.at[there], e_ssem, e_rsem.at[there], {"tm": later_k})

    for t in range(half):
        @pl.when(has_up)
        def _():
            h_up[t].start()

        @pl.when(has_down)
        def _():
            h_down[t].start()

        @pl.when(has_prior)
        def _():
            n_copy[t].start()

    pert_load.wait()
    p_copy = remote(pert_v.at[e], pert_v.at[e], p_ssem, p_rsem, partner)
    p_copy.start()

    @pl.when(jnp.logical_not(has_up))
    def _():
        h_after[...] = jnp.zeros_like(h_after)
        a_after[...] = jnp.zeros_like(a_after)

    @pl.when(jnp.logical_not(has_down))
    def _():
        h_before[...] = jnp.zeros_like(h_before)
        a_before[...] = jnp.zeros_like(a_before)

    @pl.when(jnp.logical_not(has_prior))
    def _():
        prior_v[...] = jnp.zeros_like(prior_v)

    @pl.when(jnp.logical_not(has_later))
    def _():
        nxt_v[...] = jnp.zeros_like(nxt_v)

    edge_in = ((e == 0) & has_down) | ((e == E - 1) & has_up)

    @pl.when(jnp.logical_not(edge_in))
    def _():
        edge_v[...] = jnp.zeros_like(edge_v)

    def weigh(t, rows):
        wl, wt = wide[1, t, rows], wide[2, t, rows]
        wl2, wt2 = wl * wl, wt * wt
        coef[t, 0, rows] = 1.0 - wl2 - wt2
        coef[t, 1, rows] = 0.5 * (wl2 - wl)
        coef[t, 2, rows] = 0.5 * (wl2 + wl)
        coef[t, 3, rows] = 0.5 * (wt2 - wt)
        coef[t, 4, rows] = 0.5 * (wt2 + wt)

    for t in range(half):
        weigh(t, slice(0, crow))
        for at in (1, 2):
            wide[at, t, crow : crow + 8] = jnp.zeros((8, width), jnp.float32)

    for item in small:
        item.wait()
    deep = lax.broadcasted_iota(jnp.int32, (slots, blocks), 0)
    precisions = jnp.where(deep < cnt_ref[...], prc_ref[...], 0.0)
    values = val_ref[...]
    for j in range(blocks):
        prc_b[j] = jnp.broadcast_to(precisions[:, j : j + 1], (slots, 128)).reshape(slots // 8, 8, 128)
        val_b[j] = jnp.broadcast_to(values[:, j : j + 1], (slots, 128)).reshape(slots // 8, 8, 128)
    column = lax.broadcasted_iota(jnp.int32, (blocks, blocks * 8), 1)
    block = lax.broadcasted_iota(jnp.int32, (blocks, blocks * 8), 0)
    spread = ((column >= block * 8) & (column < (block + 1) * 8)).astype(jnp.float32)
    rows = mm(jnp.broadcast_to(rows_ref[...].astype(jnp.float32), (8, blocks)), spread, NN, HIGHEST)[0:1]
    line = lax.broadcasted_iota(jnp.int32, (crow, blocks * 8), 0)
    for t in range(half):
        wanted = (line + level[t] * crow).astype(jnp.float32)
        pick[t] = (jnp.abs(rows - wanted) < 0.5).astype(jnp.bfloat16)

    jac_load.wait()
    if rem:
        tail[...] = jnp.zeros_like(tail)
        tail[:, :, :, 0:rem] = jac_v[:, :, :, lon - rem : lon]

    def strip(at, c):
        if rem and c == tiles - 1:
            return tail[at]
        return jac_v[at, :, :, c * 128 : (c + 1) * 128]

    def observe(t):
        def measure(base, carry):
            for u in range(4):
                j = base * 4 + u
                row = lax.rem(rows_s[0, j], crow)
                total = jnp.zeros((slots // 8, 8, 128), jnp.float32)
                for c in range(tiles):
                    total = total + strip(j, c) * lines[row, :, c * 128 : (c + 1) * 128]
                part_v[j] = total
            return carry

        lax.fori_loop(0, blocks // 4, measure, 0)
        evolved = jnp.sum(part_v[...], axis=-1, keepdims=True)
        wgt[...] = prc_b[...] * (evolved - val_b[...])
        for c in range(0, tiles, 2):
            pieces = []
            for cc in range(c, min(c + 2, tiles)):
                piece = jnp.sum(strip(slice(None), cc) * wgt[...], axis=1)
                pieces.append(piece.reshape(blocks * 8, 128))
            hi, lo = split(jnp.concatenate(pieces, axis=1))
            adj[t, 0:crow, c * 128 : c * 128 + hi.shape[1]] = mm(pick[t], hi, NN) + mm(pick[t], lo, NN)

    def back(t):
        g = adj[t]
        return (
            coef[t, 0] * g
            + turn(coef[t, 1] * g, 1, 1)
            + turn(coef[t, 2] * g, -1, 1)
            + turn(coef[t, 3] * g, 1, 0)
            + turn(coef[t, 4] * g, -1, 0)
        )

    def owner_copy(t, h):
        return remote(forc.at[t * E + h], rs_v.at[k], rs_ssem, rs_rsem, {"tm": level[t], "ens": h})

    def edge_copy(t, h, device):
        return remote(edge.at[h, t], edge_v.at[k], ed_ssem.at[h], ed_rsem, device)

    edge_up = [edge_copy(t, 0, {"tm": level[t], "lat": lax.rem(b + 1, L), "ens": 0}) for t in range(half)]
    edge_down = [edge_copy(t, 1, {"tm": level[t], "lat": lax.rem(b + L - 1, L), "ens": E - 1}) for t in range(half)]

    for t in range(half):
        @pl.when(has_down)
        def _():
            h_up[t].wait_recv()

        @pl.when(has_up)
        def _():
            h_down[t].wait_recv()

        wide[0, t, crow : crow + 2] = h_after[t, 0]
        wide[0, t, crow + 2 : crow + 4] = h_after[t, 1]
        wide[0, t, crow + 4 : crow + 6] = h_before[t, 0]
        wide[0, t, crow + 6 : crow + 8] = h_before[t, 1]
        for at in (1, 2):
            wide[at, t, crow : crow + 2] = h_after[t, 1 + at]
            wide[at, t, crow + 2 : crow + 3] = h_after[t, 4, at - 1 : at]
            wide[at, t, crow + 5 : crow + 6] = h_before[t, 4, at - 1 : at]
            wide[at, t, crow + 6 : crow + 8] = h_before[t, 1 + at]
        weigh(t, slice(crow, crow + 8))
        for _ in range(STEPS):
            f = wide[0, t]
            wide[0, t] = (
                coef[t, 0] * f
                + coef[t, 1] * turn(f, -1, 1)
                + coef[t, 2] * turn(f, 1, 1)
                + coef[t, 3] * turn(f, -1, 0)
                + coef[t, 4] * turn(f, 1, 0)
            )
        end_v[t] = wide[0, t, 0:crow]
        for r in range(crow):
            lines[r] = wide[0, t, r : r + 1]
        observe(t)
        @pl.when(has_later)
        def _():
            n_copy[t].wait_recv()

        scale = jnp.where(has_later, mp_ref[level[t]], 0.0)
        adj[t, 0:crow, 0:lon] = adj[t, 0:crow, 0:lon] - scale * (nxt_v[t] - end_v[t, :, 0:lon])
        extend(adj, (t,), lon)
        adj[t, crow : crow + 8] = jnp.zeros((8, width), jnp.float32)
        for h in range(E):
            forc[t * E + h] = adj[t, h * 8 : h * 8 + 8]
        rim = jnp.zeros((8, width), jnp.float32)
        for _ in range(STEPS - 1):
            adj[t] = back(t)
            for h in range(E):
                forc[t * E + h] += adj[t, h * 8 : h * 8 + 8]
            rim = rim + adj[t, crow : crow + 8]
        edge[0, t] = rim[0:4]
        edge[1, t] = rim[4:8]

        @pl.when(has_up)
        def _():
            edge_up[t].start()

        @pl.when(has_down)
        def _():
            edge_down[t].start()

        for h in range(E):
            here = (k == level[t]) & (e == h)

            @pl.when(here)
            def _():
                rs_v[k] = forc[t * E + h]

            @pl.when(jnp.logical_not(here))
            def _():
                owner_copy(t, h).start()

    for t in range(half):
        adj[t] = back(t)
        a_up_v[t] = adj[t, crow : crow + 4]
        a_down_v[t] = adj[t, crow + 4 : crow + 8]
    a_up = remote(a_up_v, a_before, a_ssem.at[0], a_rsem.at[0], up)
    a_down = remote(a_down_v, a_after, a_ssem.at[1], a_rsem.at[1], down)

    @pl.when(has_up)
    def _():
        a_up.start()

    @pl.when(has_down)
    def _():
        a_down.start()

    owner = k // half == e

    def all_but(ref, some):
        return ref.at[pl.ds(0, ref.shape[0] - some)]

    for some, when in ((1, owner), (0, jnp.logical_not(owner))):
        @pl.when(when)
        def _():
            remote(all_but(forc, some), all_but(forc, some), rs_ssem, rs_rsem, partner).wait_send()

    @pl.when(has_later)
    def _():
        for t in range(half):
            e_copy(t).start()

    p_copy.wait_recv()
    for some, when in ((1, owner), (0, jnp.logical_not(owner))):
        @pl.when(when)
        def _():
            remote(all_but(rs_v, some), all_but(rs_v, some), rs_ssem, rs_rsem, partner).wait_recv()

    @pl.when(edge_in)
    def _():
        remote(edge_v, edge_v, ed_ssem.at[0], ed_rsem, partner).wait_recv()

    total, rim = rs_v[0], edge_v[0]
    for at in range(1, T):
        total = total + rs_v[at]
        rim = rim + edge_v[at]
    line = lax.broadcasted_iota(jnp.int32, (8, width), 0)
    rim = jnp.concatenate([rim, rim], axis=0)
    total = total + jnp.where((line < 4) == (e == 0), rim, 0.0)
    total = total[:, 0:lon]
    lane = lax.broadcasted_iota(jnp.int32, (8, 128), 1)
    part = jnp.zeros((8, 128), jnp.float32)
    for m in range(E * members):
        dots = jnp.sum(pert_v[m // members, m % members, e] * total, axis=1, keepdims=True)
        part = jnp.where(lane == m, dots, part)
    part = jnp.sum(part, axis=0, keepdims=True)
    ca_send[...] = part
    if direct:
        crowd = [(dt, db, de) for dt in range(T) for db in range(L) for de in range(E) if dt or db or de]
        pl.semaphore_wait(all_sem, L - 1)
    else:
        crowd = [(dt, 0, de) for dt, de in group]

    def seat(dt, db, de):
        at, lat, ens = lax.rem(k + dt, T), lax.rem(b + db, L), lax.rem(e + de, E)
        index = (at * L + lat) * E + ens if direct else at * E + ens
        return index, {"tm": at, "lat": lat, "ens": ens}

    sums = cb_v if direct else ca_v
    me, _ = seat(0, 0, 0)
    sums[me] = part
    for dt, db, de in crowd:
        remote(ca_send, sums.at[me], ca_ssem, ca_rsem, seat(dt, db, de)[1]).start()

    @pl.when(has_prior)
    def _():
        for t in range(half):
            remote(end_v.at[t], prior_v.at[t], e_ssem, e_rsem.at[t], partner).wait_recv()

    @pl.when(has_down)
    def _():
        a_up.wait_recv()

    @pl.when(has_up)
    def _():
        a_down.wait_recv()

    for t in range(half):
        prec = mp_ref[level[t]]
        gap = jnp.zeros((crow - 8, lon), jnp.float32)
        rims = jnp.concatenate([a_before[t][:, 0:lon], gap, a_after[t][:, 0:lon]], axis=0)
        grad_v[level[t]] = adj[t, 0:crow, 0:lon] + rims + prec * (fields[0, t] - prior_v[t, :, 0:lon])
    g_copy = remote(grad_v.at[own], grad_v.at[own], g_ssem, g_rsem, partner)
    g_copy.start()
    others = sums.at[pl.ds(0, len(crowd))]
    remote(others, others, ca_ssem, ca_rsem, partner).wait_recv()
    if not direct:
        part = ca_v[0]
        for at in range(1, T * E):
            part = part + ca_v[at]
        cb_send[...] = part
        cb_v[b] = part
        for db in range(1, L):
            remote(cb_send, cb_v.at[b], cb_ssem, cb_rsem, {"lat": lax.rem(b + db, L)}).start()
        bands = remote(all_but(cb_v, 1), all_but(cb_v, 1), cb_ssem, cb_rsem, partner)
        bands.wait_recv()
    g_copy.wait_recv()

    @pl.when(has_up)
    def _():
        remote(h_last, h_before, h_ssem.at[0], h_rsem.at[0, 0], up).wait_send()
        a_up.wait_send()
        remote(edge.at[0], edge.at[0], ed_ssem.at[0], ed_rsem, up).wait_send()

    @pl.when(has_down)
    def _():
        remote(h_first, h_after, h_ssem.at[1], h_rsem.at[1, 0], down).wait_send()
        a_down.wait_send()
        remote(edge.at[1], edge.at[1], ed_ssem.at[1], ed_rsem, down).wait_send()

    @pl.when(has_prior)
    def _():
        remote(nxt_v, nxt_v, t_ssem, t_rsem.at[0], partner).wait_send()

    @pl.when(has_later)
    def _():
        remote(end_v, end_v, e_ssem, e_rsem.at[0], partner).wait_send()

    p_copy.wait_send()
    g_copy.wait_send()
    remote(others, others, ca_ssem, ca_rsem, partner).wait_send()
    if not direct:
        bands.wait_send()


def finish(grad_v, pert_v, cb_v, grad_hbm, step_hbm, step_v, out_sem):
    g_out = pltpu.make_async_copy(grad_v, grad_hbm, out_sem.at[0])
    g_out.start()
    ens, members, rows, _, lon = pert_v.shape
    count = ens * members
    part = cb_v[0]
    for at in range(1, cb_v.shape[0]):
        part = part + cb_v[at]
    factor = jnp.broadcast_to(part, (8, 128)) * (-1.0 / (count - 1.0))
    for h in range(rows):
        mixed = jnp.zeros((8, lon), jnp.float32)
        for m in range(count):
            mixed = mixed + factor[:, m : m + 1] * pert_v[m // members, m % members, h]
        step_v[h * 8 : h * 8 + 8, :] = mixed
    s_out = pltpu.make_async_copy(step_v, step_hbm, out_sem.at[1])
    s_out.start()
    g_out.wait()
    s_out.wait()


def on_device(T, L, E, increment, wind_lon, wind_lat, model_precision, perturbations, obs_rows, obs_jacobian,
              obs_values, obs_precision, obs_counts):
    _, levels, crow, lon = increment.shape
    members = perturbations.shape[0]
    blocks, slots = obs_jacobian.shape[1:3]
    half, width = levels // E, -(-lon // 128) * 128
    heard = T * L * E if T * L * E <= 64 else L
    f32, dma = jnp.float32, pltpu.SemaphoreType.DMA
    vmem, anyw = pl.BlockSpec(memory_space=pltpu.VMEM), pl.BlockSpec(memory_space=pl.ANY)

    def buf(*shape, kind=f32):
        return pltpu.VMEM(shape, kind)

    table = buf(blocks, slots // 8, 8, 128)
    parts = pl.pallas_call(
        functools.partial(kernel, T, L, E),
        out_shape=(
            buf(levels, crow, lon),
            buf(E, members, crow // 8, 8, lon),
            buf(heard, 1, 128),
        ),
        in_specs=[pl.BlockSpec(memory_space=pltpu.HBM)] * 10,
        out_specs=(vmem, vmem, vmem),
        scratch_shapes=[
            pltpu.SMEM((1, blocks), jnp.int32), pltpu.VMEM((1, blocks), jnp.int32), pltpu.VMEM((1, blocks), jnp.int32),
            buf(slots, blocks), buf(slots, blocks), pltpu.SMEM((levels,), f32),
            buf(3, half, crow, lon), buf(blocks, slots // 8, 8, lon), table, table, table, table, table,
            buf(half, crow, blocks * 8, kind=jnp.bfloat16),
            buf(3, half, 24, width), buf(half, 5, 24, width), buf(half, 24, width),
            buf(half, 5, 2, width), buf(half, 5, 2, width), buf(half, 5, 2, width), buf(half, 5, 2, width),
            buf(half, 4, width), buf(half, 4, width), buf(half, 4, width), buf(half, 4, width),
            buf(half, crow, width), buf(crow, 1, width), buf(half, crow, lon), buf(half, crow, width),
            buf(half * E, 8, width), buf(2, half, 4, width), buf(T, 8, width), buf(T, 4, width),
            buf(1, 128), buf(T * E, 1, 128), buf(1, 128),
            dma((3,)), dma((6,)), dma((2,)), dma((2, half)), dma((2,)), dma((2,)), dma, dma((half,)), dma, dma((half,)),
            dma, dma, dma, dma, dma((2,)), dma, dma, dma, dma, dma, dma, dma, pltpu.SemaphoreType.REGULAR,
        ],
        compiler_params=pltpu.CompilerParams(
            collective_id=0, has_side_effects=True, vmem_limit_bytes=56 * 1024 * 1024
        ),
    )(
        obs_rows, obs_counts, obs_values[0].T, obs_precision[0].T, model_precision,
        increment[0], wind_lon[0], wind_lat[0],
        obs_jacobian.reshape(blocks, slots // 8, 8, lon),
        perturbations.reshape(members, crow // 8, 8, lon),
    )
    grad, step = pl.pallas_call(
        finish,
        out_shape=(
            jax.ShapeDtypeStruct((levels, crow, lon), f32),
            jax.ShapeDtypeStruct((crow, lon), f32),
        ),
        in_specs=[vmem] * 3,
        out_specs=(anyw, anyw),
        scratch_shapes=[buf(crow, lon), dma((2,))],
        compiler_params=pltpu.CompilerParams(vmem_limit_bytes=8 * 1024 * 1024),
    )(*[pltpu.with_memory_space_constraint(item, pltpu.VMEM) for item in parts])
    return grad[None], step[None]


def solution(mesh):
    T, L, E = mesh.shape["tm"], mesh.shape["lat"], mesh.shape["ens"]
    placed = (
        P("tm", None, "lat", None),
        P("tm", None, "lat", None),
        P("tm", None, "lat", None),
        P(),
        P("ens", "tm", "lat", None),
        P("tm", "lat"),
        P("tm", "lat", None, None),
        P("tm", "lat", None),
        P("tm", "lat", None),
        P("tm", "lat"),
    )
    return jax.shard_map(
        functools.partial(on_device, T, L, E),
        mesh=mesh,
        in_specs=placed,
        out_specs=(P("tm", None, "lat", None), P("tm", "lat", None)),
        check_vma=False,
    )
```

```python
import functools

import jax
import jax.numpy as jnp
from jax import lax
from jax.experimental import pallas as pl
from jax.experimental.pallas import tpu as pltpu
from jax.sharding import PartitionSpec as P

STEPS = 4
MESH = pl.DeviceIdType.MESH
HIGHEST = lax.Precision.HIGHEST
NN = (((1,), (0,)), ((), ()))


def mm(a, b, dims, precision=None):
    return lax.dot_general(a, b, dims, precision=precision, preferred_element_type=jnp.float32)


def split(value):
    hi = value.astype(jnp.bfloat16)
    lo = (value - hi.astype(jnp.float32)).astype(jnp.bfloat16)
    return hi, lo


def turn(value, steps, axis):
    return pltpu.roll(value, steps % value.shape[axis], axis)


def extend(ref, where, lon):
    width = ref.shape[-1]
    rem = lon % 128
    last = ref[where + (slice(0, 16), slice(width - 128, width))]
    before = ref[where + (slice(0, 16), slice(width - 256, width - 128))]
    first = ref[where + (slice(0, 16), slice(0, 128))]
    lane = lax.broadcasted_iota(jnp.int32, last.shape, 1)
    wrapped = jnp.where(lane < 128 - rem, turn(before, 128 - rem, 1), turn(last, 128 - rem, 1))
    right = jnp.where(lane < rem + (128 - rem) // 2, turn(first, rem, 1), wrapped)
    ref[where + (slice(0, 16), slice(width - 128, width))] = jnp.where(lane < rem, last, right)


def kernel(
    T, L, E,
    rows_hbm, cnt_hbm, val_hbm, prc_hbm, mp_hbm, inc_hbm, wlon_hbm, wlat_hbm, jac_hbm, pert_hbm,
    grad_v, pert_v, cb_v,
    rows_s, rows_ref, cnt_ref, val_ref, prc_ref, mp_ref, fields, jac_v, tail, val_b, prc_b, part_v, wgt, pick,
    wide, coef, adj, h_first, h_last, h_after, h_before, a_up_v, a_down_v, a_after, a_before,
    end_v, lines, last, rims, nxt_v, prior_v, forc, edge, rs_v, edge_v, ca_send, ca_v, cb_send,
    load_sem, small_sem, h_ssem, h_rsem, a_ssem, a_rsem, t_ssem, t_rsem, e_ssem, e_rsem, p_ssem, p_rsem,
    rs_ssem, rs_rsem, ed_ssem, ed_rsem, ca_ssem, ca_rsem, cb_ssem, cb_rsem, g_ssem, g_rsem, all_sem, round_sem, pair_sem,
):
    k, b, e = lax.axis_index("tm"), lax.axis_index("lat"), lax.axis_index("ens")
    _, half, crow, lon = fields.shape
    width = wide.shape[-1]
    members = pert_v.shape[1]
    slots, blocks = val_ref.shape
    tiles, rem = width // 128, lon % 128
    other = 1 - e

    def shift(at):
        return lax.rem(at + e + 1, half)

    def spot(t, at, there):
        return lax.rem(t + shift(at) + half - shift(there), half)

    order = [lax.rem(shift(k) + t, half) for t in range(half)]
    level = [at * E + lax.rem(e + at, E) for at in order]

    def local(src, dst, sem):
        return pltpu.make_async_copy(src, dst, sem)

    for at, ref in enumerate((inc_hbm, wlon_hbm, wlat_hbm)):
        for t in range(half):
            local(ref.at[level[t]], fields.at[at, t], load_sem.at[0]).start()
    small = [
        local(rows_hbm, rows_s, small_sem.at[0]),
        local(rows_hbm, rows_ref, small_sem.at[1]),
        local(cnt_hbm, cnt_ref, small_sem.at[2]),
        local(val_hbm, val_ref, small_sem.at[3]),
        local(prc_hbm, prc_ref, small_sem.at[4]),
        local(mp_hbm, mp_ref, small_sem.at[5]),
    ]

    barrier = pltpu.get_barrier_semaphore()
    direct = T * L * E <= 64
    group = [(dt, de) for dt in range(T) for de in range(E) if dt or de]

    def mate(dt, de):
        return {"tm": lax.rem(k + dt, T), "ens": lax.rem(e + de, E)}

    near = direct and T == 4 and E == 2
    ring = [
        ({"ens": 1 - e}, None),
        ({"tm": k + 1 - 2 * lax.rem(k, 2)}, None),
        ({"tm": lax.rem(k + 2, T)}, None),
        ({"lat": lax.rem(b + 1, L)}, b < L - 1),
        ({"lat": lax.rem(b + L - 1, L)}, b > 0),
    ]
    middle = (k == 1) | (k == 2)

    def greet(sem, extra):
        for device, when in ring + ([({"tm": T - 1 - k}, middle)] if extra else []):
            if when is None:
                pl.semaphore_signal(sem, inc=1, device_id=device, device_id_type=MESH)
            else:
                @pl.when(when)
                def _():
                    pl.semaphore_signal(sem, inc=1, device_id=device, device_id_type=MESH)

    def meet(sem, extra):
        count = 3 + (b < L - 1).astype(jnp.int32) + (b > 0).astype(jnp.int32)
        pl.semaphore_wait(sem, count + middle.astype(jnp.int32) if extra else count)

    def round_on(at):
        if near:
            meet(round_sem.at[at], False)
            if at < 2:
                greet(round_sem.at[at + 1], False)

    if near:
        greet(barrier, True)
    else:
        for dt, de in group:
            pl.semaphore_signal(barrier, inc=1, device_id=mate(dt, de), device_id_type=MESH)
        for db in range(1, L):
            pl.semaphore_signal(barrier, inc=1, device_id={"lat": lax.rem(b + db, L)}, device_id_type=MESH)

    def remote(src, dst, ssem, rsem, device):
        return pltpu.make_async_remote_copy(
            src_ref=src, dst_ref=dst, send_sem=ssem, recv_sem=rsem, device_id=device, device_id_type=MESH
        )

    up = {"lat": lax.rem(b + 1, L)}
    down = {"lat": lax.rem(b + L - 1, L)}
    later_k, prior_k = lax.rem(k + 1, T), lax.rem(k + T - 1, T)
    partner = {"ens": other}
    has_up, has_down = b < L - 1, b > 0
    has_later, has_prior = k < T - 1, k > 0

    local(fields, fields, load_sem.at[0]).wait()
    jac_load = local(jac_hbm, jac_v, load_sem.at[1])
    pert_load = local(pert_hbm, pert_v.at[e], load_sem.at[2])
    for item in small + [pert_load, jac_load]:
        item.start()
    for t in range(half):
        for at in range(3):
            wide[at, t, 0:16, 0:lon] = fields[at, t]
            extend(wide, (at, t), lon)
        h_first[t, 0] = wide[0, t, 0:2]
        h_first[t, 1] = wide[0, t, 2:4]
        h_last[t, 0] = wide[0, t, crow - 4 : crow - 2]
        h_last[t, 1] = wide[0, t, crow - 2 : crow]
        for at in (1, 2):
            h_first[t, 1 + at] = wide[at, t, 0:2]
            h_first[t, 4, at - 1 : at] = wide[at, t, 2:3]
            h_last[t, 1 + at] = wide[at, t, crow - 2 : crow]
            h_last[t, 4, at - 1 : at] = wide[at, t, crow - 3 : crow - 2]

    if near:
        meet(barrier, True)
    else:
        pl.semaphore_wait(barrier, len(group) + L - 1)
        if direct:
            for db in range(1, L):
                pl.semaphore_signal(all_sem, inc=1, device_id={"lat": lax.rem(b + db, L)}, device_id_type=MESH)

    h_up = [remote(h_last.at[t], h_before.at[t], h_ssem.at[0], h_rsem.at[0, t], up) for t in range(half)]
    h_down = [remote(h_first.at[t], h_after.at[t], h_ssem.at[1], h_rsem.at[1, t], down) for t in range(half)]
    n_copy = [
        remote(fields.at[0, spot(t, prior_k, k)], nxt_v.at[t], t_ssem, t_rsem.at[t], {"tm": prior_k})
        for t in range(half)
    ]

    def e_copy(t):
        there = spot(t, k, later_k)
        return remote(end_v.at[t], prior_v.at[there], e_ssem, e_rsem.at[there], {"tm": later_k})

    for t in range(half):
        @pl.when(has_up)
        def _():
            h_up[t].start()

        @pl.when(has_down)
        def _():
            h_down[t].start()

        @pl.when(has_prior)
        def _():
            n_copy[t].start()

    if near:
        greet(round_sem.at[0], False)
    pert_load.wait()
    p_copy = remote(pert_v.at[e], pert_v.at[e], p_ssem, p_rsem, partner)
    p_copy.start()

    @pl.when(jnp.logical_not(has_up))
    def _():
        h_after[...] = jnp.zeros_like(h_after)
        a_after[...] = jnp.zeros_like(a_after)

    @pl.when(jnp.logical_not(has_down))
    def _():
        h_before[...] = jnp.zeros_like(h_before)
        a_before[...] = jnp.zeros_like(a_before)

    @pl.when(jnp.logical_not(has_prior))
    def _():
        prior_v[...] = jnp.zeros_like(prior_v)

    @pl.when(jnp.logical_not(has_later))
    def _():
        nxt_v[...] = jnp.zeros_like(nxt_v)

    edge_in = ((e == 0) & has_down) | ((e == E - 1) & has_up)

    @pl.when(jnp.logical_not(edge_in))
    def _():
        edge_v[...] = jnp.zeros_like(edge_v)

    def weigh(t, rows):
        wl, wt = wide[1, t, rows], wide[2, t, rows]
        wl2, wt2 = wl * wl, wt * wt
        coef[t, 0, rows] = 1.0 - wl2 - wt2
        coef[t, 1, rows] = 0.5 * (wl2 - wl)
        coef[t, 2, rows] = 0.5 * (wl2 + wl)
        coef[t, 3, rows] = 0.5 * (wt2 - wt)
        coef[t, 4, rows] = 0.5 * (wt2 + wt)

    for t in range(half):
        weigh(t, slice(0, crow))
        for at in (1, 2):
            wide[at, t, crow : crow + 8] = jnp.zeros((8, width), jnp.float32)

    for item in small:
        item.wait()
    deep = lax.broadcasted_iota(jnp.int32, (slots, blocks), 0)
    precisions = jnp.where(deep < cnt_ref[...], prc_ref[...], 0.0)
    values = val_ref[...]
    for j in range(blocks):
        prc_b[j] = jnp.broadcast_to(precisions[:, j : j + 1], (slots, 128)).reshape(slots // 8, 8, 128)
        val_b[j] = jnp.broadcast_to(values[:, j : j + 1], (slots, 128)).reshape(slots // 8, 8, 128)
    column = lax.broadcasted_iota(jnp.int32, (blocks, blocks * 8), 1)
    block = lax.broadcasted_iota(jnp.int32, (blocks, blocks * 8), 0)
    spread = ((column >= block * 8) & (column < (block + 1) * 8)).astype(jnp.float32)
    rows = mm(jnp.broadcast_to(rows_ref[...].astype(jnp.float32), (8, blocks)), spread, NN, HIGHEST)[0:1]
    line = lax.broadcasted_iota(jnp.int32, (crow, blocks * 8), 0)
    for t in range(half):
        wanted = (line + level[t] * crow).astype(jnp.float32)
        pick[t] = (jnp.abs(rows - wanted) < 0.5).astype(jnp.bfloat16)

    round_on(0)
    jac_load.wait()
    if rem:
        tail[...] = jnp.zeros_like(tail)
        tail[:, :, :, 0:rem] = jac_v[:, :, :, lon - rem : lon]

    def strip(at, c):
        if rem and c == tiles - 1:
            return tail[at]
        return jac_v[at, :, :, c * 128 : (c + 1) * 128]

    def measure(t):
        def one(j):
            row = lax.rem(rows_s[0, j], crow)
            total = strip(j, 0) * lines[t, row, :, spans[0]]
            for c in range(1, tiles):
                total = total + strip(j, c) * lines[t, row, :, spans[c]]
            part_v[j] = total

        return [functools.partial(one, j) for j in range(blocks)]

    def place(t):
        evolved = jnp.sum(part_v[...], axis=-1, keepdims=True)
        wgt[...] = prc_b[...] * (evolved - val_b[...])
        for c in range(0, tiles, 2):
            pieces = []
            for cc in range(c, min(c + 2, tiles)):
                piece = jnp.sum(strip(slice(None), cc) * wgt[...], axis=1)
                pieces.append(piece.reshape(blocks * 8, 128))
            hi, lo = split(jnp.concatenate(pieces, axis=1))
            adj[t, 0:crow, c * 128 : c * 128 + hi.shape[1]] = mm(pick[t], hi, NN) + mm(pick[t], lo, NN)

    def beside(tasks, done, of):
        for task in tasks[len(tasks) * done // of : len(tasks) * (done + 1) // of]:
            task()

    lane = lax.broadcasted_iota(jnp.int32, (24, 128), 1)
    starts, stops = lane == 0, lane == 127
    spans = [slice(c * 128, (c + 1) * 128) for c in range(tiles)]

    def forward(t, src, emit):
        east = turn(src[:, spans[-1]], 1, 1)
        here = src[:, spans[0]]
        west = first_west = turn(here, -1, 1)
        for c in range(tiles):
            f, f_west, f_east = here, west, turn(here, 1, 1)
            if c + 1 < tiles:
                here = src[:, spans[c + 1]]
                west = turn(here, -1, 1)
            after = west if c + 1 < tiles else first_west
            emit(c, (
                coef[t, 0, :, spans[c]] * f
                + coef[t, 1, :, spans[c]] * jnp.where(stops, after, f_west)
                + coef[t, 2, :, spans[c]] * jnp.where(starts, east, f_east)
                + coef[t, 3, :, spans[c]] * turn(f, -1, 0)
                + coef[t, 4, :, spans[c]] * turn(f, 1, 0)
            ))
            east = f_east

    def back(t, src, emit):
        def moved(c):
            g = src[:, spans[c]]
            return g, turn(coef[t, 1, :, spans[c]] * g, 1, 1), turn(coef[t, 2, :, spans[c]] * g, -1, 1)

        east = moved(tiles - 1)[1]
        now = first = moved(0)
        for c in range(tiles):
            g, g_east, g_west = now
            if c + 1 < tiles:
                now = moved(c + 1)
            after = now[2] if c + 1 < tiles else first[2]
            emit(c, (
                coef[t, 0, :, spans[c]] * g
                + jnp.where(starts, east, g_east)
                + jnp.where(stops, after, g_west)
                + turn(coef[t, 3, :, spans[c]] * g, 1, 0)
                + turn(coef[t, 4, :, spans[c]] * g, -1, 0)
            ))
            east = g_east

    def owner_copy(t, h):
        return remote(forc.at[t * E + h], rs_v.at[k], rs_ssem, rs_rsem, {"tm": level[t], "ens": h})

    def edge_copy(t, h, device):
        return remote(edge.at[h, t], edge_v.at[k], ed_ssem.at[h], ed_rsem, device)

    edge_up = [edge_copy(t, 0, {"tm": level[t], "lat": lax.rem(b + 1, L), "ens": 0}) for t in range(half)]
    edge_down = [edge_copy(t, 1, {"tm": level[t], "lat": lax.rem(b + L - 1, L), "ens": E - 1}) for t in range(half)]

    pairs = [(wide.at[0, t], adj.at[t]) for t in range(half)]

    def advance(t, tasks):
        @pl.when(has_down)
        def _():
            h_up[t].wait_recv()

        @pl.when(has_up)
        def _():
            h_down[t].wait_recv()

        wide[0, t, crow : crow + 2] = h_after[t, 0]
        wide[0, t, crow + 2 : crow + 4] = h_after[t, 1]
        wide[0, t, crow + 4 : crow + 6] = h_before[t, 0]
        wide[0, t, crow + 6 : crow + 8] = h_before[t, 1]
        for at in (1, 2):
            wide[at, t, crow : crow + 2] = h_after[t, 1 + at]
            wide[at, t, crow + 2 : crow + 3] = h_after[t, 4, at - 1 : at]
            wide[at, t, crow + 5 : crow + 6] = h_before[t, 4, at - 1 : at]
            wide[at, t, crow + 6 : crow + 8] = h_before[t, 1 + at]
        weigh(t, slice(crow, crow + 8))
        for at in range(STEPS):
            src, dst = pairs[t][at % 2], pairs[t][(at + 1) % 2]

            def emit(c, value):
                if at + 1 < STEPS:
                    dst[:, spans[c]] = value
                else:
                    end_v[t, :, spans[c]] = value[0:crow]
                    for r in range(crow):
                        lines[t, r, :, spans[c]] = value[r : r + 1]
                beside(tasks, at * tiles + c, STEPS * tiles)

            forward(t, src, emit)

    def retreat(t, tasks):
        scale = jnp.where(has_later, mp_ref[level[t]], 0.0)
        adj[t, 0:crow, 0:lon] = adj[t, 0:crow, 0:lon] - scale * (nxt_v[t] - end_v[t, :, 0:lon])
        extend(adj, (t,), lon)
        adj[t, crow : crow + 8] = jnp.zeros((8, width), jnp.float32)
        for at in range(STEPS - 1):
            src, dst = pairs[t][(at + 1) % 2], pairs[t][at % 2]

            def emit(c, value):
                dst[:, spans[c]] = value
                for h in range(E):
                    rows = slice(h * 8, h * 8 + 8)
                    base = adj[t, rows, spans[c]] if at == 0 else forc[t * E + h, :, spans[c]]
                    forc[t * E + h, :, spans[c]] = base + value[rows]
                rim = value[crow:] if at == 0 else rims[:, spans[c]] + value[crow:]
                if at < STEPS - 2:
                    rims[:, spans[c]] = rim
                else:
                    edge[0, t, :, spans[c]] = rim[0:4]
                    edge[1, t, :, spans[c]] = rim[4:8]
                beside(tasks, at * tiles + c, (STEPS - 1) * tiles)

            back(t, src, emit)

    round_on(1)
    advance(0, [])
    for t in range(half):
        if t < half // 2:
            @pl.when(has_later)
            def _():
                e_copy(t).start()

        first_tasks = measure(t) if t == 0 else []
        if t + 1 < half:
            advance(t + 1, first_tasks)
        else:
            for task in first_tasks:
                task()
        place(t)
        @pl.when(has_later)
        def _():
            n_copy[t].wait_recv()

        retreat(t, measure(t + 1) if t + 1 < half else [])
        if t == 0:
            round_on(2)
        @pl.when(has_up)
        def _():
            edge_up[t].start()

        @pl.when(has_down)
        def _():
            edge_down[t].start()

        for h in range(E):
            here = (k == level[t]) & (e == h)

            @pl.when(here)
            def _():
                rs_v[k] = forc[t * E + h]

            @pl.when(jnp.logical_not(here))
            def _():
                owner_copy(t, h).start()

    owner = lax.rem(k + E * half - k // E, E) == e

    def all_but(ref, some):
        return ref.at[pl.ds(0, ref.shape[0] - some)]

    def sent_all():
        for some, when in ((1, owner), (0, jnp.logical_not(owner))):
            @pl.when(when)
            def _():
                remote(all_but(forc, some), all_but(forc, some), rs_ssem, rs_rsem, partner).wait_send()

    def send_end():
        for t in range(half // 2, half):
            e_copy(t).start()

    @pl.when(has_later & (k != 1))
    def _():
        send_end()

    for t in range(half):
        def emit(c, value):
            last[t, :, spans[c]] = value[0:crow]
            a_up_v[t, :, spans[c]] = value[crow : crow + 4]
            a_down_v[t, :, spans[c]] = value[crow + 4 :]

        back(t, (adj.at[t], wide.at[0, t])[STEPS % 2 == 0], emit)
    a_up = remote(a_up_v, a_before, a_ssem.at[0], a_rsem.at[0], up)
    a_down = remote(a_down_v, a_after, a_ssem.at[1], a_rsem.at[1], down)

    @pl.when(has_up)
    def _():
        a_up.start()

    @pl.when(has_down)
    def _():
        a_down.start()

    @pl.when(k == 1)
    def _():
        sent_all()

        @pl.when(e == 0)
        def _():
            pl.semaphore_signal(pair_sem, inc=1, device_id=partner, device_id_type=MESH)

        @pl.when(e != 0)
        def _():
            pl.semaphore_wait(pair_sem, 1)

        @pl.when(has_later)
        def _():
            send_end()

    p_copy.wait_recv()
    for some, when in ((1, owner), (0, jnp.logical_not(owner))):
        @pl.when(when)
        def _():
            remote(all_but(rs_v, some), all_but(rs_v, some), rs_ssem, rs_rsem, partner).wait_recv()

    @pl.when(edge_in)
    def _():
        remote(edge_v, edge_v, ed_ssem.at[0], ed_rsem, partner).wait_recv()

    total, rim = rs_v[0], edge_v[0]
    for at in range(1, T):
        total = total + rs_v[at]
        rim = rim + edge_v[at]
    line = lax.broadcasted_iota(jnp.int32, (8, width), 0)
    rim = jnp.concatenate([rim, rim], axis=0)
    total = total + jnp.where((line < 4) == (e == 0), rim, 0.0)
    total = total[:, 0:lon]
    lane = lax.broadcasted_iota(jnp.int32, (8, 128), 1)
    part = jnp.zeros((8, 128), jnp.float32)
    for m in range(E * members):
        dots = jnp.sum(pert_v[m // members, m % members, e] * total, axis=1, keepdims=True)
        part = jnp.where(lane == m, dots, part)
    part = jnp.sum(part, axis=0, keepdims=True)
    ca_send[...] = part
    if direct:
        crowd = [(dt, lat, de) for lat in range(L) for dt in range(T) for de in range(E)]
        if not near:
            pl.semaphore_wait(all_sem, L - 1)
    else:
        crowd = [(dt, b, de) for dt, de in group]

    def seat(dt, lat, de):
        at, ens = lax.rem(k + dt, T), lax.rem(e + de, E)
        index = (at * L + lat) * E + ens if direct else at * E + ens
        return index, {"tm": at, "lat": lat, "ens": ens}

    sums = cb_v if direct else ca_v
    me, _ = seat(0, b, 0)
    sums[me] = part
    for dt, lat, de in crowd:
        copy = remote(ca_send, sums.at[me], ca_ssem, ca_rsem, seat(dt, lat, de)[1])
        if dt or de:
            copy.start()
        else:
            @pl.when(lat != b)
            def _():
                copy.start()

    @pl.when(has_prior)
    def _():
        for t in range(half):
            remote(end_v.at[t], prior_v.at[t], e_ssem, e_rsem.at[t], partner).wait_recv()

    @pl.when(has_down)
    def _():
        a_up.wait_recv()

    @pl.when(has_up)
    def _():
        a_down.wait_recv()

    for t in range(half):
        prec = mp_ref[level[t]]
        gap = jnp.zeros((crow - 8, lon), jnp.float32)
        rims_in = jnp.concatenate([a_before[t][:, 0:lon], gap, a_after[t][:, 0:lon]], axis=0)
        grad_v[level[t]] = last[t, :, 0:lon] + rims_in + prec * (fields[0, t] - prior_v[t, :, 0:lon])
        remote(grad_v.at[level[t]], grad_v.at[level[t]], g_ssem, g_rsem, partner).start()
    grad_half = grad_v.at[pl.ds(0, half)]
    g_copy = remote(grad_half, grad_half, g_ssem, g_rsem, partner)
    others = all_but(sums, 1)
    remote(others, others, ca_ssem, ca_rsem, partner).wait_recv()
    if not direct:
        part = ca_v[0]
        for at in range(1, T * E):
            part = part + ca_v[at]
        cb_send[...] = part
        cb_v[b] = part
        for db in range(1, L):
            remote(cb_send, cb_v.at[b], cb_ssem, cb_rsem, {"lat": lax.rem(b + db, L)}).start()
        bands = remote(all_but(cb_v, 1), all_but(cb_v, 1), cb_ssem, cb_rsem, partner)
        bands.wait_recv()
    g_copy.wait_recv()

    @pl.when(k != 1)
    def _():
        sent_all()

    @pl.when(has_up)
    def _():
        remote(h_last, h_before, h_ssem.at[0], h_rsem.at[0, 0], up).wait_send()
        a_up.wait_send()
        remote(edge.at[0], edge.at[0], ed_ssem.at[0], ed_rsem, up).wait_send()

    @pl.when(has_down)
    def _():
        remote(h_first, h_after, h_ssem.at[1], h_rsem.at[1, 0], down).wait_send()
        a_down.wait_send()
        remote(edge.at[1], edge.at[1], ed_ssem.at[1], ed_rsem, down).wait_send()

    @pl.when(has_prior)
    def _():
        remote(nxt_v, nxt_v, t_ssem, t_rsem.at[0], partner).wait_send()

    @pl.when(has_later)
    def _():
        remote(end_v, end_v, e_ssem, e_rsem.at[0], partner).wait_send()

    p_copy.wait_send()
    g_copy.wait_send()
    remote(others, others, ca_ssem, ca_rsem, partner).wait_send()
    if not direct:
        bands.wait_send()


def finish(grad_v, pert_v, cb_v, grad_hbm, step_hbm, step_v, out_sem):
    g_out = pltpu.make_async_copy(grad_v, grad_hbm, out_sem.at[0])
    g_out.start()
    ens, members, rows, _, lon = pert_v.shape
    count = ens * members
    part = cb_v[0]
    for at in range(1, cb_v.shape[0]):
        part = part + cb_v[at]
    factor = jnp.broadcast_to(part, (8, 128)) * (-1.0 / (count - 1.0))
    for h in range(rows):
        mixed = jnp.zeros((8, lon), jnp.float32)
        for m in range(count):
            mixed = mixed + factor[:, m : m + 1] * pert_v[m // members, m % members, h]
        step_v[h * 8 : h * 8 + 8, :] = mixed
    s_out = pltpu.make_async_copy(step_v, step_hbm, out_sem.at[1])
    s_out.start()
    g_out.wait()
    s_out.wait()


def on_device(T, L, E, increment, wind_lon, wind_lat, model_precision, perturbations, obs_rows, obs_jacobian,
              obs_values, obs_precision, obs_counts):
    _, levels, crow, lon = increment.shape
    members = perturbations.shape[0]
    blocks, slots = obs_jacobian.shape[1:3]
    half, width = levels // E, -(-lon // 128) * 128
    heard = T * L * E if T * L * E <= 64 else L
    f32, dma = jnp.float32, pltpu.SemaphoreType.DMA
    vmem, anyw = pl.BlockSpec(memory_space=pltpu.VMEM), pl.BlockSpec(memory_space=pl.ANY)

    def buf(*shape, kind=f32):
        return pltpu.VMEM(shape, kind)

    table = buf(blocks, slots // 8, 8, 128)
    parts = pl.pallas_call(
        functools.partial(kernel, T, L, E),
        out_shape=(
            buf(levels, crow, lon),
            buf(E, members, crow // 8, 8, lon),
            buf(heard, 1, 128),
        ),
        in_specs=[pl.BlockSpec(memory_space=pltpu.HBM)] * 10,
        out_specs=(vmem, vmem, vmem),
        scratch_shapes=[
            pltpu.SMEM((1, blocks), jnp.int32), pltpu.VMEM((1, blocks), jnp.int32), pltpu.VMEM((1, blocks), jnp.int32),
            buf(slots, blocks), buf(slots, blocks), pltpu.SMEM((levels,), f32),
            buf(3, half, crow, lon), buf(blocks, slots // 8, 8, lon), table, table, table, table, table,
            buf(half, crow, blocks * 8, kind=jnp.bfloat16),
            buf(3, half, 24, width), buf(half, 5, 24, width), buf(half, 24, width),
            buf(half, 5, 2, width), buf(half, 5, 2, width), buf(half, 5, 2, width), buf(half, 5, 2, width),
            buf(half, 4, width), buf(half, 4, width), buf(half, 4, width), buf(half, 4, width),
            buf(half, crow, width), buf(half, crow, 1, width), buf(half, crow, width), buf(8, width), buf(half, crow, lon), buf(half, crow, width),
            buf(half * E, 8, width), buf(2, half, 4, width), buf(T, 8, width), buf(T, 4, width),
            buf(1, 128), buf(T * E, 1, 128), buf(1, 128),
            dma((3,)), dma((6,)), dma((2,)), dma((2, half)), dma((2,)), dma((2,)), dma, dma((half,)), dma, dma((half,)),
            dma, dma, dma, dma, dma((2,)), dma, dma, dma, dma, dma, dma, dma, pltpu.SemaphoreType.REGULAR,
            pltpu.SemaphoreType.REGULAR((3,)), pltpu.SemaphoreType.REGULAR,
        ],
        compiler_params=pltpu.CompilerParams(
            collective_id=0, has_side_effects=True, vmem_limit_bytes=56 * 1024 * 1024
        ),
    )(
        obs_rows, obs_counts, obs_values[0].T, obs_precision[0].T, model_precision,
        increment[0], wind_lon[0], wind_lat[0],
        obs_jacobian.reshape(blocks, slots // 8, 8, lon),
        perturbations.reshape(members, crow // 8, 8, lon),
    )
    grad, step = pl.pallas_call(
        finish,
        out_shape=(
            jax.ShapeDtypeStruct((levels, crow, lon), f32),
            jax.ShapeDtypeStruct((crow, lon), f32),
        ),
        in_specs=[vmem] * 3,
        out_specs=(anyw, anyw),
        scratch_shapes=[buf(crow, lon), dma((2,))],
        compiler_params=pltpu.CompilerParams(vmem_limit_bytes=8 * 1024 * 1024),
    )(*[pltpu.with_memory_space_constraint(item, pltpu.VMEM) for item in parts])
    return grad[None], step[None]


def solution(mesh):
    T, L, E = mesh.shape["tm"], mesh.shape["lat"], mesh.shape["ens"]
    placed = (
        P("tm", None, "lat", None),
        P("tm", None, "lat", None),
        P("tm", None, "lat", None),
        P(),
        P("ens", "tm", "lat", None),
        P("tm", "lat"),
        P("tm", "lat", None, None),
        P("tm", "lat", None),
        P("tm", "lat", None),
        P("tm", "lat"),
    )
    return jax.shard_map(
        functools.partial(on_device, T, L, E),
        mesh=mesh,
        in_specs=placed,
        out_specs=(P("tm", None, "lat", None), P("tm", "lat", None)),
        check_vma=False,
    )
```

```python
import functools

import jax
import jax.numpy as jnp
from jax import lax
from jax.experimental import pallas as pl
from jax.experimental.pallas import tpu as pltpu
from jax.sharding import PartitionSpec as P

STEPS = 4
MESH = pl.DeviceIdType.MESH
HIGHEST = lax.Precision.HIGHEST
NN = (((1,), (0,)), ((), ()))


def mm(a, b, dims, precision=None):
    return lax.dot_general(a, b, dims, precision=precision, preferred_element_type=jnp.float32)


def split(value):
    hi = value.astype(jnp.bfloat16)
    lo = (value - hi.astype(jnp.float32)).astype(jnp.bfloat16)
    return hi, lo


def turn(value, steps, axis):
    return pltpu.roll(value, steps % value.shape[axis], axis)


def extend(ref, where, lon):
    width = ref.shape[-1]
    rem = lon % 128
    last = ref[where + (slice(0, 16), slice(width - 128, width))]
    before = ref[where + (slice(0, 16), slice(width - 256, width - 128))]
    first = ref[where + (slice(0, 16), slice(0, 128))]
    lane = lax.broadcasted_iota(jnp.int32, last.shape, 1)
    wrapped = jnp.where(lane < 128 - rem, turn(before, 128 - rem, 1), turn(last, 128 - rem, 1))
    right = jnp.where(lane < rem + (128 - rem) // 2, turn(first, rem, 1), wrapped)
    ref[where + (slice(0, 16), slice(width - 128, width))] = jnp.where(lane < rem, last, right)


def kernel(
    T, L, E,
    rows_hbm, cnt_hbm, val_hbm, prc_hbm, mp_hbm, inc_hbm, wlon_hbm, wlat_hbm, jac_hbm, pert_hbm,
    grad_v, pert_v, cb_v,
    rows_s, rows_ref, cnt_ref, val_ref, prc_ref, mp_ref, fields, jac_v, tail, val_b, prc_b, part_v, wgt, pick,
    wide, coef, adj, h_first, h_last, h_after, h_before, a_up_v, a_down_v, a_after, a_before,
    end_v, lines, last, rims, nxt_v, prior_v, forc, edge, rs_v, edge_v, ca_send, ca_v, cb_send,
    load_sem, small_sem, h_ssem, h_rsem, a_ssem, a_rsem, t_ssem, t_rsem, e_ssem, e_rsem, p_ssem, p_rsem,
    rs_ssem, rs_rsem, ed_ssem, ed_rsem, ca_ssem, ca_rsem, cb_ssem, cb_rsem, g_ssem, g_rsem, all_sem, round_sem, pair_sem,
):
    k, b, e = lax.axis_index("tm"), lax.axis_index("lat"), lax.axis_index("ens")
    _, half, crow, lon = fields.shape
    width = wide.shape[-1]
    members = pert_v.shape[1]
    slots, blocks = val_ref.shape
    tiles, rem = width // 128, lon % 128
    other = 1 - e

    def shift(at):
        return lax.rem(at + e + 1, half)

    def spot(t, at, there):
        return lax.rem(t + shift(at) + half - shift(there), half)

    order = [lax.rem(shift(k) + t, half) for t in range(half)]
    level = [at * E + lax.rem(e + at, E) for at in order]

    def local(src, dst, sem):
        return pltpu.make_async_copy(src, dst, sem)

    for at, ref in enumerate((inc_hbm, wlon_hbm, wlat_hbm)):
        for t in range(half):
            local(ref.at[level[t]], fields.at[at, t], load_sem.at[0]).start()
    small = [
        local(rows_hbm, rows_s, small_sem.at[0]),
        local(rows_hbm, rows_ref, small_sem.at[1]),
        local(cnt_hbm, cnt_ref, small_sem.at[2]),
        local(val_hbm, val_ref, small_sem.at[3]),
        local(prc_hbm, prc_ref, small_sem.at[4]),
        local(mp_hbm, mp_ref, small_sem.at[5]),
    ]

    barrier = pltpu.get_barrier_semaphore()
    direct = T * L * E <= 64
    group = [(dt, de) for dt in range(T) for de in range(E) if dt or de]

    def mate(dt, de):
        return {"tm": lax.rem(k + dt, T), "ens": lax.rem(e + de, E)}

    near = direct and T == 4 and E == 2
    ring = [
        ({"ens": 1 - e}, None),
        ({"tm": k + 1 - 2 * lax.rem(k, 2)}, None),
        ({"tm": lax.rem(k + 2, T)}, None),
        ({"lat": lax.rem(b + 1, L)}, b < L - 1),
        ({"lat": lax.rem(b + L - 1, L)}, b > 0),
    ]
    middle = (k == 1) | (k == 2)

    def greet(sem, extra):
        for device, when in ring + ([({"tm": T - 1 - k}, middle)] if extra else []):
            if when is None:
                pl.semaphore_signal(sem, inc=1, device_id=device, device_id_type=MESH)
            else:
                @pl.when(when)
                def _():
                    pl.semaphore_signal(sem, inc=1, device_id=device, device_id_type=MESH)

    def meet(sem, extra):
        count = 3 + (b < L - 1).astype(jnp.int32) + (b > 0).astype(jnp.int32)
        pl.semaphore_wait(sem, count + middle.astype(jnp.int32) if extra else count)

    def round_on(at):
        if near:
            meet(round_sem.at[at], False)
            if at < 2:
                greet(round_sem.at[at + 1], False)

    if near:
        greet(barrier, True)
    else:
        for dt, de in group:
            pl.semaphore_signal(barrier, inc=1, device_id=mate(dt, de), device_id_type=MESH)
        for db in range(1, L):
            pl.semaphore_signal(barrier, inc=1, device_id={"lat": lax.rem(b + db, L)}, device_id_type=MESH)

    def remote(src, dst, ssem, rsem, device):
        return pltpu.make_async_remote_copy(
            src_ref=src, dst_ref=dst, send_sem=ssem, recv_sem=rsem, device_id=device, device_id_type=MESH
        )

    up = {"lat": lax.rem(b + 1, L)}
    down = {"lat": lax.rem(b + L - 1, L)}
    later_k, prior_k = lax.rem(k + 1, T), lax.rem(k + T - 1, T)
    partner = {"ens": other}
    has_up, has_down = b < L - 1, b > 0
    has_later, has_prior = k < T - 1, k > 0

    local(fields, fields, load_sem.at[0]).wait()
    jac_load = local(jac_hbm, jac_v, load_sem.at[1])
    pert_load = local(pert_hbm, pert_v.at[e], load_sem.at[2])
    for item in small + [pert_load, jac_load]:
        item.start()
    for t in range(half):
        for at in range(3):
            wide[at, t, 0:16, 0:lon] = fields[at, t]
            extend(wide, (at, t), lon)
        h_first[t, 0] = wide[0, t, 0:2]
        h_first[t, 1] = wide[0, t, 2:4]
        h_last[t, 0] = wide[0, t, crow - 4 : crow - 2]
        h_last[t, 1] = wide[0, t, crow - 2 : crow]
        for at in (1, 2):
            h_first[t, 1 + at] = wide[at, t, 0:2]
            h_first[t, 4, at - 1 : at] = wide[at, t, 2:3]
            h_last[t, 1 + at] = wide[at, t, crow - 2 : crow]
            h_last[t, 4, at - 1 : at] = wide[at, t, crow - 3 : crow - 2]

    if near:
        meet(barrier, True)
    else:
        pl.semaphore_wait(barrier, len(group) + L - 1)
        if direct:
            for db in range(1, L):
                pl.semaphore_signal(all_sem, inc=1, device_id={"lat": lax.rem(b + db, L)}, device_id_type=MESH)

    h_up = [remote(h_last.at[t], h_before.at[t], h_ssem.at[0], h_rsem.at[0, t], up) for t in range(half)]
    h_down = [remote(h_first.at[t], h_after.at[t], h_ssem.at[1], h_rsem.at[1, t], down) for t in range(half)]
    n_copy = [
        remote(fields.at[0, spot(t, prior_k, k)], nxt_v.at[t], t_ssem, t_rsem.at[t], {"tm": prior_k})
        for t in range(half)
    ]

    def e_copy(t):
        there = spot(t, k, later_k)
        return remote(end_v.at[t], prior_v.at[there], e_ssem, e_rsem.at[there], {"tm": later_k})

    for t in range(half):
        @pl.when(has_up)
        def _():
            h_up[t].start()

        @pl.when(has_down)
        def _():
            h_down[t].start()

        @pl.when(has_prior)
        def _():
            n_copy[t].start()

    if near:
        greet(round_sem.at[0], False)
    pert_load.wait()
    p_copy = remote(pert_v.at[e], pert_v.at[e], p_ssem, p_rsem, partner)
    p_copy.start()

    @pl.when(jnp.logical_not(has_up))
    def _():
        h_after[...] = jnp.zeros_like(h_after)
        a_after[...] = jnp.zeros_like(a_after)

    @pl.when(jnp.logical_not(has_down))
    def _():
        h_before[...] = jnp.zeros_like(h_before)
        a_before[...] = jnp.zeros_like(a_before)

    @pl.when(jnp.logical_not(has_prior))
    def _():
        prior_v[...] = jnp.zeros_like(prior_v)

    @pl.when(jnp.logical_not(has_later))
    def _():
        nxt_v[...] = jnp.zeros_like(nxt_v)

    edge_in = ((e == 0) & has_down) | ((e == E - 1) & has_up)

    @pl.when(jnp.logical_not(edge_in))
    def _():
        edge_v[...] = jnp.zeros_like(edge_v)

    def weigh(t, rows):
        wl, wt = wide[1, t, rows], wide[2, t, rows]
        wl2, wt2 = wl * wl, wt * wt
        coef[t, 0, rows] = 1.0 - wl2 - wt2
        coef[t, 1, rows] = 0.5 * (wl2 - wl)
        coef[t, 2, rows] = 0.5 * (wl2 + wl)
        coef[t, 3, rows] = 0.5 * (wt2 - wt)
        coef[t, 4, rows] = 0.5 * (wt2 + wt)

    for t in range(half):
        weigh(t, slice(0, crow))
        for at in (1, 2):
            wide[at, t, crow : crow + 8] = jnp.zeros((8, width), jnp.float32)

    for item in small:
        item.wait()
    deep = lax.broadcasted_iota(jnp.int32, (slots, blocks), 0)
    precisions = jnp.where(deep < cnt_ref[...], prc_ref[...], 0.0)
    values = val_ref[...]
    for j in range(blocks):
        prc_b[j] = jnp.broadcast_to(precisions[:, j : j + 1], (slots, 128)).reshape(slots // 8, 8, 128)
        val_b[j] = jnp.broadcast_to(values[:, j : j + 1], (slots, 128)).reshape(slots // 8, 8, 128)
    column = lax.broadcasted_iota(jnp.int32, (blocks, blocks * 8), 1)
    block = lax.broadcasted_iota(jnp.int32, (blocks, blocks * 8), 0)
    spread = ((column >= block * 8) & (column < (block + 1) * 8)).astype(jnp.float32)
    rows = mm(jnp.broadcast_to(rows_ref[...].astype(jnp.float32), (8, blocks)), spread, NN, HIGHEST)[0:1]
    line = lax.broadcasted_iota(jnp.int32, (crow, blocks * 8), 0)
    for t in range(half):
        wanted = (line + level[t] * crow).astype(jnp.float32)
        pick[t * crow : (t + 1) * crow] = (jnp.abs(rows - wanted) < 0.5).astype(jnp.bfloat16)

    round_on(0)
    jac_load.wait()
    if rem:
        tail[...] = jnp.zeros_like(tail)
        tail[:, :, :, 0:rem] = jac_v[:, :, :, lon - rem : lon]

    def strip(at, c):
        if rem and c == tiles - 1:
            return tail[at]
        return jac_v[at, :, :, c * 128 : (c + 1) * 128]

    def observe():
        def measure(base, carry):
            for u in range(8):
                j = base * 8 + u
                row = rows_s[0, j]
                slot = lax.rem(row // (crow * E) + half - shift(k), half)
                row = lax.rem(row, crow)
                total = strip(j, 0) * lines[slot, row, :, spans[0]]
                for c in range(1, tiles):
                    total = total + strip(j, c) * lines[slot, row, :, spans[c]]
                part_v[j] = total
            return carry

        lax.fori_loop(0, blocks // 8, measure, 0)
        evolved = jnp.sum(part_v[...], axis=-1, keepdims=True)
        wgt[...] = prc_b[...] * (evolved - val_b[...])
        for c in range(0, tiles, 2):
            pieces = []
            for cc in range(c, min(c + 2, tiles)):
                piece = jnp.sum(strip(slice(None), cc) * wgt[...], axis=1)
                pieces.append(piece.reshape(blocks * 8, 128))
            hi, lo = split(jnp.concatenate(pieces, axis=1))
            placed = mm(pick[...], hi, NN) + mm(pick[...], lo, NN)
            for t in range(half):
                adj[t, 0:crow, c * 128 : c * 128 + hi.shape[1]] = placed[t * crow : (t + 1) * crow]

    lane = lax.broadcasted_iota(jnp.int32, (24, 128), 1)
    starts, stops = lane == 0, lane == 127
    spans = [slice(c * 128, (c + 1) * 128) for c in range(tiles)]

    def forward(t, src, emit):
        east = turn(src[:, spans[-1]], 1, 1)
        here = src[:, spans[0]]
        west = first_west = turn(here, -1, 1)
        for c in range(tiles):
            f, f_west, f_east = here, west, turn(here, 1, 1)
            if c + 1 < tiles:
                here = src[:, spans[c + 1]]
                west = turn(here, -1, 1)
            after = west if c + 1 < tiles else first_west
            emit(c, (
                coef[t, 0, :, spans[c]] * f
                + coef[t, 1, :, spans[c]] * jnp.where(stops, after, f_west)
                + coef[t, 2, :, spans[c]] * jnp.where(starts, east, f_east)
                + coef[t, 3, :, spans[c]] * turn(f, -1, 0)
                + coef[t, 4, :, spans[c]] * turn(f, 1, 0)
            ))
            east = f_east

    def back(t, src, emit):
        def moved(c):
            g = src[:, spans[c]]
            return g, turn(coef[t, 1, :, spans[c]] * g, 1, 1), turn(coef[t, 2, :, spans[c]] * g, -1, 1)

        east = moved(tiles - 1)[1]
        now = first = moved(0)
        for c in range(tiles):
            g, g_east, g_west = now
            if c + 1 < tiles:
                now = moved(c + 1)
            after = now[2] if c + 1 < tiles else first[2]
            emit(c, (
                coef[t, 0, :, spans[c]] * g
                + jnp.where(starts, east, g_east)
                + jnp.where(stops, after, g_west)
                + turn(coef[t, 3, :, spans[c]] * g, 1, 0)
                + turn(coef[t, 4, :, spans[c]] * g, -1, 0)
            ))
            east = g_east

    def owner_copy(t, h):
        return remote(forc.at[t * E + h], rs_v.at[k], rs_ssem, rs_rsem, {"tm": level[t], "ens": h})

    def edge_copy(t, h, device):
        return remote(edge.at[h, t], edge_v.at[k], ed_ssem.at[h], ed_rsem, device)

    edge_up = [edge_copy(t, 0, {"tm": level[t], "lat": lax.rem(b + 1, L), "ens": 0}) for t in range(half)]
    edge_down = [edge_copy(t, 1, {"tm": level[t], "lat": lax.rem(b + L - 1, L), "ens": E - 1}) for t in range(half)]

    pairs = [(wide.at[0, t], adj.at[t]) for t in range(half)]

    def advance(t):
        @pl.when(has_down)
        def _():
            h_up[t].wait_recv()

        @pl.when(has_up)
        def _():
            h_down[t].wait_recv()

        wide[0, t, crow : crow + 2] = h_after[t, 0]
        wide[0, t, crow + 2 : crow + 4] = h_after[t, 1]
        wide[0, t, crow + 4 : crow + 6] = h_before[t, 0]
        wide[0, t, crow + 6 : crow + 8] = h_before[t, 1]
        for at in (1, 2):
            wide[at, t, crow : crow + 2] = h_after[t, 1 + at]
            wide[at, t, crow + 2 : crow + 3] = h_after[t, 4, at - 1 : at]
            wide[at, t, crow + 5 : crow + 6] = h_before[t, 4, at - 1 : at]
            wide[at, t, crow + 6 : crow + 8] = h_before[t, 1 + at]
        weigh(t, slice(crow, crow + 8))
        for at in range(STEPS):
            src, dst = pairs[t][at % 2], pairs[t][(at + 1) % 2]

            def emit(c, value):
                if at + 1 < STEPS:
                    dst[:, spans[c]] = value
                else:
                    end_v[t, :, spans[c]] = value[0:crow]
                    for r in range(crow):
                        lines[t, r, :, spans[c]] = value[r : r + 1]

            forward(t, src, emit)

    def retreat(t):
        scale = jnp.where(has_later, mp_ref[level[t]], 0.0)
        adj[t, 0:crow, 0:lon] = adj[t, 0:crow, 0:lon] - scale * (nxt_v[t] - end_v[t, :, 0:lon])
        extend(adj, (t,), lon)
        adj[t, crow : crow + 8] = jnp.zeros((8, width), jnp.float32)
        for at in range(STEPS - 1):
            src, dst = pairs[t][(at + 1) % 2], pairs[t][at % 2]

            def emit(c, value):
                dst[:, spans[c]] = value
                for h in range(E):
                    rows = slice(h * 8, h * 8 + 8)
                    base = adj[t, rows, spans[c]] if at == 0 else forc[t * E + h, :, spans[c]]
                    forc[t * E + h, :, spans[c]] = base + value[rows]
                rim = value[crow:] if at == 0 else rims[:, spans[c]] + value[crow:]
                if at < STEPS - 2:
                    rims[:, spans[c]] = rim
                else:
                    for r in range(3):
                        edge[0, t, r, :, spans[c]] = rim[r : r + 1]
                        edge[1, t, r, :, spans[c]] = rim[r + 5 : r + 6]

            back(t, src, emit)

    round_on(1)
    for t in range(half):
        advance(t)
        if t < half // 2:
            @pl.when(has_later)
            def _():
                e_copy(t).start()

    observe()
    for t in range(half):
        @pl.when(has_later)
        def _():
            n_copy[t].wait_recv()

        retreat(t)
        if t == 0:
            round_on(2)
        @pl.when(has_up)
        def _():
            edge_up[t].start()

        @pl.when(has_down)
        def _():
            edge_down[t].start()

        for h in range(E):
            here = (k == level[t]) & (e == h)

            @pl.when(here)
            def _():
                rs_v[k] = forc[t * E + h]

            @pl.when(jnp.logical_not(here))
            def _():
                owner_copy(t, h).start()

    owner = lax.rem(k + E * half - k // E, E) == e

    def all_but(ref, some):
        return ref.at[pl.ds(0, ref.shape[0] - some)]

    def sent_all():
        for some, when in ((1, owner), (0, jnp.logical_not(owner))):
            @pl.when(when)
            def _():
                remote(all_but(forc, some), all_but(forc, some), rs_ssem, rs_rsem, partner).wait_send()

    def send_end():
        for t in range(half // 2, half):
            e_copy(t).start()

    @pl.when(has_later & (k != 1))
    def _():
        send_end()

    for t in range(half):
        def emit(c, value):
            last[t, :, spans[c]] = value[0:crow]
            a_up_v[t, :, spans[c]] = value[crow : crow + 4]
            a_down_v[t, :, spans[c]] = value[crow + 4 :]

        back(t, (adj.at[t], wide.at[0, t])[STEPS % 2 == 0], emit)
    a_up = remote(a_up_v, a_before, a_ssem.at[0], a_rsem.at[0], up)
    a_down = remote(a_down_v, a_after, a_ssem.at[1], a_rsem.at[1], down)

    @pl.when(has_up)
    def _():
        a_up.start()

    @pl.when(has_down)
    def _():
        a_down.start()

    @pl.when(k == 1)
    def _():
        sent_all()

        @pl.when(e == 0)
        def _():
            pl.semaphore_signal(pair_sem, inc=1, device_id=partner, device_id_type=MESH)

        @pl.when(e != 0)
        def _():
            pl.semaphore_wait(pair_sem, 1)

        @pl.when(has_later)
        def _():
            send_end()

    p_copy.wait_recv()
    for some, when in ((1, owner), (0, jnp.logical_not(owner))):
        @pl.when(when)
        def _():
            remote(all_but(rs_v, some), all_but(rs_v, some), rs_ssem, rs_rsem, partner).wait_recv()

    @pl.when(edge_in)
    def _():
        remote(edge_v, edge_v, ed_ssem.at[0], ed_rsem, partner).wait_recv()

    total = rs_v[0]
    for at in range(1, T):
        total = total + rs_v[at]
    inner = [sum((edge_v[at, r] for at in range(1, T)), edge_v[0, r]) for r in range(3)]
    blank = jnp.zeros((5, width), jnp.float32)
    total = total + jnp.where(
        e == 0, jnp.concatenate(inner + [blank], axis=0), jnp.concatenate([blank] + inner, axis=0)
    )
    total = total[:, 0:lon]
    lane = lax.broadcasted_iota(jnp.int32, (8, 128), 1)
    part = jnp.zeros((8, 128), jnp.float32)
    for m in range(E * members):
        dots = jnp.sum(pert_v[m // members, m % members, e] * total, axis=1, keepdims=True)
        part = jnp.where(lane == m, dots, part)
    part = jnp.sum(part, axis=0, keepdims=True)
    ca_send[...] = part
    if direct:
        crowd = [(dt, lat, de) for lat in range(L) for dt in range(T) for de in range(E)]
        if not near:
            pl.semaphore_wait(all_sem, L - 1)
    else:
        crowd = [(dt, b, de) for dt, de in group]

    def seat(dt, lat, de):
        at, ens = lax.rem(k + dt, T), lax.rem(e + de, E)
        index = (at * L + lat) * E + ens if direct else at * E + ens
        return index, {"tm": at, "lat": lat, "ens": ens}

    sums = cb_v if direct else ca_v
    me, _ = seat(0, b, 0)
    sums[me] = part
    for dt, lat, de in crowd:
        copy = remote(ca_send, sums.at[me], ca_ssem, ca_rsem, seat(dt, lat, de)[1])
        if dt or de:
            copy.start()
        else:
            @pl.when(lat != b)
            def _():
                copy.start()

    @pl.when(has_prior)
    def _():
        for t in range(half):
            remote(end_v.at[t], prior_v.at[t], e_ssem, e_rsem.at[t], partner).wait_recv()

    @pl.when(has_down)
    def _():
        a_up.wait_recv()

    @pl.when(has_up)
    def _():
        a_down.wait_recv()

    for t in range(half):
        prec = mp_ref[level[t]]
        gap = jnp.zeros((crow - 8, lon), jnp.float32)
        rims_in = jnp.concatenate([a_before[t][:, 0:lon], gap, a_after[t][:, 0:lon]], axis=0)
        grad_v[level[t]] = last[t, :, 0:lon] + rims_in + prec * (fields[0, t] - prior_v[t, :, 0:lon])
        remote(grad_v.at[level[t]], grad_v.at[level[t]], g_ssem, g_rsem, partner).start()
    grad_half = grad_v.at[pl.ds(0, half)]
    g_copy = remote(grad_half, grad_half, g_ssem, g_rsem, partner)
    others = all_but(sums, 1)
    remote(others, others, ca_ssem, ca_rsem, partner).wait_recv()
    if not direct:
        part = ca_v[0]
        for at in range(1, T * E):
            part = part + ca_v[at]
        cb_send[...] = part
        cb_v[b] = part
        for db in range(1, L):
            remote(cb_send, cb_v.at[b], cb_ssem, cb_rsem, {"lat": lax.rem(b + db, L)}).start()
        bands = remote(all_but(cb_v, 1), all_but(cb_v, 1), cb_ssem, cb_rsem, partner)
        bands.wait_recv()
    g_copy.wait_recv()

    @pl.when(k != 1)
    def _():
        sent_all()

    @pl.when(has_up)
    def _():
        remote(h_last, h_before, h_ssem.at[0], h_rsem.at[0, 0], up).wait_send()
        a_up.wait_send()
        remote(edge.at[0], edge.at[0], ed_ssem.at[0], ed_rsem, up).wait_send()

    @pl.when(has_down)
    def _():
        remote(h_first, h_after, h_ssem.at[1], h_rsem.at[1, 0], down).wait_send()
        a_down.wait_send()
        remote(edge.at[1], edge.at[1], ed_ssem.at[1], ed_rsem, down).wait_send()

    @pl.when(has_prior)
    def _():
        remote(nxt_v, nxt_v, t_ssem, t_rsem.at[0], partner).wait_send()

    @pl.when(has_later)
    def _():
        remote(end_v, end_v, e_ssem, e_rsem.at[0], partner).wait_send()

    p_copy.wait_send()
    g_copy.wait_send()
    remote(others, others, ca_ssem, ca_rsem, partner).wait_send()
    if not direct:
        bands.wait_send()


def finish(grad_v, pert_v, cb_v, grad_hbm, step_hbm, step_v, out_sem):
    g_out = pltpu.make_async_copy(grad_v, grad_hbm, out_sem.at[0])
    g_out.start()
    ens, members, rows, _, lon = pert_v.shape
    count = ens * members
    part = cb_v[0]
    for at in range(1, cb_v.shape[0]):
        part = part + cb_v[at]
    factor = jnp.broadcast_to(part, (8, 128)) * (-1.0 / (count - 1.0))
    for h in range(rows):
        mixed = jnp.zeros((8, lon), jnp.float32)
        for m in range(count):
            mixed = mixed + factor[:, m : m + 1] * pert_v[m // members, m % members, h]
        step_v[h * 8 : h * 8 + 8, :] = mixed
    s_out = pltpu.make_async_copy(step_v, step_hbm, out_sem.at[1])
    s_out.start()
    g_out.wait()
    s_out.wait()


def on_device(T, L, E, increment, wind_lon, wind_lat, model_precision, perturbations, obs_rows, obs_jacobian,
              obs_values, obs_precision, obs_counts):
    _, levels, crow, lon = increment.shape
    members = perturbations.shape[0]
    blocks, slots = obs_jacobian.shape[1:3]
    half, width = levels // E, -(-lon // 128) * 128
    heard = T * L * E if T * L * E <= 64 else L
    f32, dma = jnp.float32, pltpu.SemaphoreType.DMA
    vmem, anyw = pl.BlockSpec(memory_space=pltpu.VMEM), pl.BlockSpec(memory_space=pl.ANY)

    def buf(*shape, kind=f32):
        return pltpu.VMEM(shape, kind)

    table = buf(blocks, slots // 8, 8, 128)
    parts = pl.pallas_call(
        functools.partial(kernel, T, L, E),
        out_shape=(
            buf(levels, crow, lon),
            buf(E, members, crow // 8, 8, lon),
            buf(heard, 1, 128),
        ),
        in_specs=[pl.BlockSpec(memory_space=pltpu.HBM)] * 10,
        out_specs=(vmem, vmem, vmem),
        scratch_shapes=[
            pltpu.SMEM((1, blocks), jnp.int32), pltpu.VMEM((1, blocks), jnp.int32), pltpu.VMEM((1, blocks), jnp.int32),
            buf(slots, blocks), buf(slots, blocks), pltpu.SMEM((levels,), f32),
            buf(3, half, crow, lon), buf(blocks, slots // 8, 8, lon), table, table, table, table, table,
            buf(half * crow, blocks * 8, kind=jnp.bfloat16),
            buf(3, half, 24, width), buf(half, 5, 24, width), buf(half, 24, width),
            buf(half, 5, 2, width), buf(half, 5, 2, width), buf(half, 5, 2, width), buf(half, 5, 2, width),
            buf(half, 4, width), buf(half, 4, width), buf(half, 4, width), buf(half, 4, width),
            buf(half, crow, width), buf(half, crow, 1, width), buf(half, crow, width), buf(8, width), buf(half, crow, lon), buf(half, crow, width),
            buf(half * E, 8, width), buf(2, half, 3, 1, width), buf(T, 8, width), buf(T, 3, 1, width),
            buf(1, 128), buf(T * E, 1, 128), buf(1, 128),
            dma((3,)), dma((6,)), dma((2,)), dma((2, half)), dma((2,)), dma((2,)), dma, dma((half,)), dma, dma((half,)),
            dma, dma, dma, dma, dma((2,)), dma, dma, dma, dma, dma, dma, dma, pltpu.SemaphoreType.REGULAR,
            pltpu.SemaphoreType.REGULAR((3,)), pltpu.SemaphoreType.REGULAR,
        ],
        compiler_params=pltpu.CompilerParams(
            collective_id=0, has_side_effects=True, vmem_limit_bytes=56 * 1024 * 1024
        ),
    )(
        obs_rows, obs_counts, obs_values[0].T, obs_precision[0].T, model_precision,
        increment[0], wind_lon[0], wind_lat[0],
        obs_jacobian.reshape(blocks, slots // 8, 8, lon),
        perturbations.reshape(members, crow // 8, 8, lon),
    )
    grad, step = pl.pallas_call(
        finish,
        out_shape=(
            jax.ShapeDtypeStruct((levels, crow, lon), f32),
            jax.ShapeDtypeStruct((crow, lon), f32),
        ),
        in_specs=[vmem] * 3,
        out_specs=(anyw, anyw),
        scratch_shapes=[buf(crow, lon), dma((2,))],
        compiler_params=pltpu.CompilerParams(vmem_limit_bytes=8 * 1024 * 1024),
    )(*[pltpu.with_memory_space_constraint(item, pltpu.VMEM) for item in parts])
    return grad[None], step[None]


def solution(mesh):
    T, L, E = mesh.shape["tm"], mesh.shape["lat"], mesh.shape["ens"]
    placed = (
        P("tm", None, "lat", None),
        P("tm", None, "lat", None),
        P("tm", None, "lat", None),
        P(),
        P("ens", "tm", "lat", None),
        P("tm", "lat"),
        P("tm", "lat", None, None),
        P("tm", "lat", None),
        P("tm", "lat", None),
        P("tm", "lat"),
    )
    return jax.shard_map(
        functools.partial(on_device, T, L, E),
        mesh=mesh,
        in_specs=placed,
        out_specs=(P("tm", None, "lat", None), P("tm", "lat", None)),
        check_vma=False,
    )
```

```python
import functools

import jax
import jax.numpy as jnp
from jax import lax
from jax.experimental import pallas as pl
from jax.experimental.pallas import tpu as pltpu
from jax.sharding import PartitionSpec as P

STEPS = 4
MESH = pl.DeviceIdType.MESH
HIGHEST = lax.Precision.HIGHEST
NN = (((1,), (0,)), ((), ()))


def mm(a, b, dims, precision=None):
    return lax.dot_general(a, b, dims, precision=precision, preferred_element_type=jnp.float32)


def split(value):
    hi = value.astype(jnp.bfloat16)
    lo = (value - hi.astype(jnp.float32)).astype(jnp.bfloat16)
    return hi, lo


def turn(value, steps, axis):
    return pltpu.roll(value, steps % value.shape[axis], axis)


def extend(ref, where, lon):
    width = ref.shape[-1]
    rem = lon % 128
    last = ref[where + (slice(0, 16), slice(width - 128, width))]
    before = ref[where + (slice(0, 16), slice(width - 256, width - 128))]
    first = ref[where + (slice(0, 16), slice(0, 128))]
    lane = lax.broadcasted_iota(jnp.int32, last.shape, 1)
    wrapped = jnp.where(lane < 128 - rem, turn(before, 128 - rem, 1), turn(last, 128 - rem, 1))
    right = jnp.where(lane < rem + (128 - rem) // 2, turn(first, rem, 1), wrapped)
    ref[where + (slice(0, 16), slice(width - 128, width))] = jnp.where(lane < rem, last, right)


def kernel(
    T, L, E,
    rows_hbm, cnt_hbm, val_hbm, prc_hbm, mp_hbm, inc_hbm, wlon_hbm, wlat_hbm, jac_hbm, pert_hbm,
    grad_v, pert_v, cb_v,
    rows_s, whole_ref, slot_ref, mp_ref, fields, jac_v, tail, val_b, prc_b, part_v, wgt, pick,
    wide, coef, adj, h_first, h_last, h_after, h_before, a_up_v, a_down_v, a_after, a_before,
    end_v, lines, last, rims, nxt_v, prior_v, forc, edge, rs_v, edge_v, ca_send, ca_v, cb_send,
    load_sem, small_sem, h_ssem, h_rsem, a_ssem, a_rsem, t_ssem, t_rsem, e_ssem, e_rsem, p_ssem, p_rsem,
    rs_ssem, rs_rsem, ed_ssem, ed_rsem, ca_ssem, ca_rsem, cb_ssem, cb_rsem, g_rsem, all_sem, round_sem,
):
    k, b, e = lax.axis_index("tm"), lax.axis_index("lat"), lax.axis_index("ens")
    _, half, crow, lon = fields.shape
    width = wide.shape[-1]
    members = pert_v.shape[1]
    _, slots, blocks = slot_ref.shape
    tiles, rem = width // 128, lon % 128
    other = 1 - e

    direct = T * L * E <= 64
    near = direct and T == 4 and E == 2
    role = lax.rem(e + k // 2, 2) if near else e

    def shift(at, core):
        return lax.rem(at + 1 + core, half)

    def keeper(at):
        return lax.rem(e + k // 2 + at // 2, 2) if near else e

    def spot(t, at, core, there, other_core):
        return lax.rem(t + shift(at, core) + half - shift(there, other_core), half)

    order = [lax.rem(shift(k, e) + t, half) for t in range(half)]
    level = [role * half + at for at in order]

    def local(src, dst, sem):
        return pltpu.make_async_copy(src, dst, sem)

    for at, ref in enumerate((inc_hbm, wlon_hbm, wlat_hbm)):
        for t in range(half):
            local(ref.at[level[t]], fields.at[at, t], load_sem.at[0]).start()
    small = [
        local(rows_hbm, rows_s, small_sem.at[0]),
        local(rows_hbm, whole_ref.at[0], small_sem.at[1]),
        local(cnt_hbm, whole_ref.at[1], small_sem.at[1]),
        local(val_hbm, slot_ref.at[0], small_sem.at[2]),
        local(prc_hbm, slot_ref.at[1], small_sem.at[2]),
        local(mp_hbm, mp_ref, small_sem.at[3]),
    ]

    barrier = pltpu.get_barrier_semaphore()
    group = [(dt, de) for dt in range(T) for de in range(E) if dt or de]

    def mate(dt, de):
        return {"tm": lax.rem(k + dt, T), "ens": lax.rem(e + de, E)}

    ring = [
        ({"ens": 1 - e}, None),
        ({"tm": k + 1 - 2 * lax.rem(k, 2)}, None),
        ({"tm": lax.rem(k + 2, T)}, None),
        ({"lat": lax.rem(b + 1, L)}, b < L - 1),
        ({"lat": lax.rem(b + L - 1, L)}, b > 0),
    ]
    middle = (k == 1) | (k == 2)

    def greet(sem, extra):
        for device, when in ring + ([({"tm": T - 1 - k, "ens": other}, middle)] if extra else []):
            if when is None:
                pl.semaphore_signal(sem, inc=1, device_id=device, device_id_type=MESH)
            else:
                @pl.when(when)
                def _():
                    pl.semaphore_signal(sem, inc=1, device_id=device, device_id_type=MESH)

    def meet(sem, extra):
        count = 3 + (b < L - 1).astype(jnp.int32) + (b > 0).astype(jnp.int32)
        pl.semaphore_wait(sem, count + middle.astype(jnp.int32) if extra else count)

    def round_on(at):
        if near:
            meet(round_sem.at[at % 2], False)
            if at < 2:
                greet(round_sem.at[(at + 1) % 2], False)

    if near:
        greet(barrier, True)
    else:
        for dt, de in group:
            pl.semaphore_signal(barrier, inc=1, device_id=mate(dt, de), device_id_type=MESH)
        for db in range(1, L):
            pl.semaphore_signal(barrier, inc=1, device_id={"lat": lax.rem(b + db, L)}, device_id_type=MESH)

    def remote(src, dst, ssem, rsem, device):
        return pltpu.make_async_remote_copy(
            src_ref=src, dst_ref=dst, send_sem=ssem, recv_sem=rsem, device_id=device, device_id_type=MESH
        )

    up = {"lat": lax.rem(b + 1, L)}
    down = {"lat": lax.rem(b + L - 1, L)}
    later_k, prior_k = lax.rem(k + 1, T), lax.rem(k + T - 1, T)
    partner = {"ens": other}
    has_up, has_down = b < L - 1, b > 0
    has_later, has_prior = k < T - 1, k > 0

    local(fields, fields, load_sem.at[0]).wait()
    jac_load = local(jac_hbm, jac_v, load_sem.at[0])
    pert_load = local(pert_hbm, pert_v.at[e], load_sem.at[1])
    for item in small + [pert_load, jac_load]:
        item.start()
    for t in range(half):
        for at in range(3):
            wide[at, t, 0:16, 0:lon] = fields[at, t]
            extend(wide, (at, t), lon)
        h_first[t, 0] = wide[0, t, 0:2]
        h_first[t, 1] = wide[0, t, 2:4]
        h_last[t, 0] = wide[0, t, crow - 4 : crow - 2]
        h_last[t, 1] = wide[0, t, crow - 2 : crow]
        for at in (1, 2):
            h_first[t, 1 + at] = wide[at, t, 0:2]
            h_first[t, 4, at - 1 : at] = wide[at, t, 2:3]
            h_last[t, 1 + at] = wide[at, t, crow - 2 : crow]
            h_last[t, 4, at - 1 : at] = wide[at, t, crow - 3 : crow - 2]

    if near:
        meet(barrier, True)
    else:
        pl.semaphore_wait(barrier, len(group) + L - 1)
        if direct:
            for db in range(1, L):
                pl.semaphore_signal(all_sem, inc=1, device_id={"lat": lax.rem(b + db, L)}, device_id_type=MESH)

    h_up = [remote(h_last.at[t], h_before.at[t], h_ssem.at[0], h_rsem.at[0, t], up) for t in range(half)]
    h_down = [remote(h_first.at[t], h_after.at[t], h_ssem.at[1], h_rsem.at[1, t], down) for t in range(half)]
    n_copy = [
        remote(fields.at[0, spot(t, prior_k, keeper(prior_k), k, e)], nxt_v.at[t], t_ssem, t_rsem.at[t], {"tm": prior_k, "ens": keeper(prior_k)})
        for t in range(half)
    ]

    def e_copy(t):
        there = spot(t, k, e, later_k, keeper(later_k))
        return remote(end_v.at[t], prior_v.at[there], e_ssem, e_rsem, {"tm": later_k, "ens": keeper(later_k)})

    for t in range(half):
        @pl.when(has_up)
        def _():
            h_up[t].start()

        @pl.when(has_down)
        def _():
            h_down[t].start()

    for t in range(half):
        @pl.when(has_prior)
        def _():
            n_copy[t].start()

    if near:
        greet(round_sem.at[0], False)
    pert_load.wait()
    p_copy = remote(pert_v.at[e], pert_v.at[e], p_ssem, p_rsem, partner)

    @pl.when(jnp.logical_not(has_up))
    def _():
        h_after[...] = jnp.zeros_like(h_after)
        a_after[...] = jnp.zeros_like(a_after)

    @pl.when(jnp.logical_not(has_down))
    def _():
        h_before[...] = jnp.zeros_like(h_before)
        a_before[...] = jnp.zeros_like(a_before)

    @pl.when(jnp.logical_not(has_prior))
    def _():
        prior_v[...] = jnp.zeros_like(prior_v)

    @pl.when(jnp.logical_not(has_later))
    def _():
        nxt_v[...] = jnp.zeros_like(nxt_v)

    edge_in = ((e == 0) & has_down) | ((e == E - 1) & has_up)

    @pl.when(jnp.logical_not(edge_in))
    def _():
        edge_v[...] = jnp.zeros_like(edge_v)

    def weigh(t, rows):
        wl, wt = wide[1, t, rows], wide[2, t, rows]
        wl2, wt2 = wl * wl, wt * wt
        coef[t, 0, rows] = 1.0 - wl2 - wt2
        coef[t, 1, rows] = 0.5 * (wl2 - wl)
        coef[t, 2, rows] = 0.5 * (wl2 + wl)
        coef[t, 3, rows] = 0.5 * (wt2 - wt)
        coef[t, 4, rows] = 0.5 * (wt2 + wt)

    for t in range(half):
        weigh(t, slice(0, crow))
        for at in (1, 2):
            wide[at, t, crow : crow + 8] = jnp.zeros((8, width), jnp.float32)

    for item in (
        small[0], small[-1], local(whole_ref, whole_ref, small_sem.at[1]), local(slot_ref, slot_ref, small_sem.at[2])
    ):
        item.wait()
    deep = lax.broadcasted_iota(jnp.int32, (slots, blocks), 0)
    precisions = jnp.where(deep < whole_ref[1], slot_ref[1], 0.0)
    values = slot_ref[0]
    for j in range(blocks):
        prc_b[j] = jnp.broadcast_to(precisions[:, j : j + 1], (slots, 128)).reshape(slots // 8, 8, 128)
        val_b[j] = jnp.broadcast_to(values[:, j : j + 1], (slots, 128)).reshape(slots // 8, 8, 128)
    column = lax.broadcasted_iota(jnp.int32, (blocks, blocks * 8), 1)
    block = lax.broadcasted_iota(jnp.int32, (blocks, blocks * 8), 0)
    spread = ((column >= block * 8) & (column < (block + 1) * 8)).astype(jnp.float32)
    rows = mm(jnp.broadcast_to(whole_ref[0].astype(jnp.float32), (8, blocks)), spread, NN, HIGHEST)[0:1]
    line = lax.broadcasted_iota(jnp.int32, (crow, blocks * 8), 0)
    for t in range(half):
        wanted = (line + level[t] * crow).astype(jnp.float32)
        pick[t * crow : (t + 1) * crow] = (jnp.abs(rows - wanted) < 0.5).astype(jnp.bfloat16)

    round_on(0)
    jac_load.wait()
    if rem:
        tail[...] = jnp.zeros_like(tail)
        tail[:, :, :, 0:rem] = jac_v[:, :, :, lon - rem : lon]

    def strip(at, c):
        if rem and c == tiles - 1:
            return tail[at]
        return jac_v[at, :, :, c * 128 : (c + 1) * 128]

    def observe():
        def measure(base, carry):
            for u in range(8):
                j = base * 8 + u
                row = rows_s[0, j]
                slot = lax.rem(row // crow + half - shift(k, e), half)
                row = lax.rem(row, crow)
                total = strip(j, 0) * lines[slot, row, :, spans[0]]
                for c in range(1, tiles):
                    total = total + strip(j, c) * lines[slot, row, :, spans[c]]
                part_v[j] = total
            return carry

        lax.fori_loop(0, blocks // 8, measure, 0)
        evolved = jnp.sum(part_v[...], axis=-1, keepdims=True)
        wgt[...] = prc_b[...] * (evolved - val_b[...])
        for c in range(0, tiles, 2):
            pieces = []
            for cc in range(c, min(c + 2, tiles)):
                piece = jnp.sum(strip(slice(None), cc) * wgt[...], axis=1)
                pieces.append(piece.reshape(blocks * 8, 128))
            hi, lo = split(jnp.concatenate(pieces, axis=1))
            placed = mm(pick[...], hi, NN) + mm(pick[...], lo, NN)
            for t in range(half):
                adj[t, 0:crow, c * 128 : c * 128 + hi.shape[1]] = placed[t * crow : (t + 1) * crow]

    lane = lax.broadcasted_iota(jnp.int32, (24, 128), 1)
    starts, stops = lane == 0, lane == 127
    spans = [slice(c * 128, (c + 1) * 128) for c in range(tiles)]

    def forward(t, src, emit):
        east = turn(src[:, spans[-1]], 1, 1)
        here = src[:, spans[0]]
        west = first_west = turn(here, -1, 1)
        for c in range(tiles):
            f, f_west, f_east = here, west, turn(here, 1, 1)
            if c + 1 < tiles:
                here = src[:, spans[c + 1]]
                west = turn(here, -1, 1)
            after = west if c + 1 < tiles else first_west
            emit(c, (
                coef[t, 0, :, spans[c]] * f
                + coef[t, 1, :, spans[c]] * jnp.where(stops, after, f_west)
                + coef[t, 2, :, spans[c]] * jnp.where(starts, east, f_east)
                + coef[t, 3, :, spans[c]] * turn(f, -1, 0)
                + coef[t, 4, :, spans[c]] * turn(f, 1, 0)
            ))
            east = f_east

    def back(t, src, emit):
        def moved(c):
            g = src[:, spans[c]]
            return g, turn(coef[t, 1, :, spans[c]] * g, 1, 1), turn(coef[t, 2, :, spans[c]] * g, -1, 1)

        east = moved(tiles - 1)[1]
        now = first = moved(0)
        for c in range(tiles):
            g, g_east, g_west = now
            if c + 1 < tiles:
                now = moved(c + 1)
            after = now[2] if c + 1 < tiles else first[2]
            emit(c, (
                coef[t, 0, :, spans[c]] * g
                + jnp.where(starts, east, g_east)
                + jnp.where(stops, after, g_west)
                + turn(coef[t, 3, :, spans[c]] * g, 1, 0)
                + turn(coef[t, 4, :, spans[c]] * g, -1, 0)
            ))
            east = g_east

    def owner_copy(t, h):
        return remote(forc.at[t * E + h], rs_v.at[k], rs_ssem, rs_rsem, {"tm": level[t], "ens": h})

    def edge_copy(t, h, device):
        return remote(edge.at[h, t], edge_v.at[k], ed_ssem.at[h], ed_rsem, device)

    edge_up = [edge_copy(t, 0, {"tm": level[t], "lat": lax.rem(b + 1, L), "ens": 0}) for t in range(half)]
    edge_down = [edge_copy(t, 1, {"tm": level[t], "lat": lax.rem(b + L - 1, L), "ens": E - 1}) for t in range(half)]

    pairs = [(wide.at[0, t], adj.at[t]) for t in range(half)]

    def advance(t):
        @pl.when(has_down)
        def _():
            h_up[t].wait_recv()

        @pl.when(has_up)
        def _():
            h_down[t].wait_recv()

        wide[0, t, crow : crow + 2] = h_after[t, 0]
        wide[0, t, crow + 2 : crow + 4] = h_after[t, 1]
        wide[0, t, crow + 4 : crow + 6] = h_before[t, 0]
        wide[0, t, crow + 6 : crow + 8] = h_before[t, 1]
        for at in (1, 2):
            wide[at, t, crow : crow + 2] = h_after[t, 1 + at]
            wide[at, t, crow + 2 : crow + 3] = h_after[t, 4, at - 1 : at]
            wide[at, t, crow + 5 : crow + 6] = h_before[t, 4, at - 1 : at]
            wide[at, t, crow + 6 : crow + 8] = h_before[t, 1 + at]
        weigh(t, slice(crow, crow + 8))
        for at in range(STEPS):
            src, dst = pairs[t][at % 2], pairs[t][(at + 1) % 2]

            def emit(c, value):
                if at + 1 < STEPS:
                    dst[:, spans[c]] = value
                else:
                    end_v[t, :, spans[c]] = value[0:crow]
                    for r in range(crow):
                        lines[t, r, :, spans[c]] = value[r : r + 1]

            forward(t, src, emit)

    def retreat(t):
        scale = jnp.where(has_later, mp_ref[level[t]], 0.0)
        adj[t, 0:crow, 0:lon] = adj[t, 0:crow, 0:lon] - scale * (nxt_v[t] - end_v[t, :, 0:lon])
        extend(adj, (t,), lon)
        adj[t, crow : crow + 8] = jnp.zeros((8, width), jnp.float32)
        for at in range(STEPS - 1):
            src, dst = pairs[t][(at + 1) % 2], pairs[t][at % 2]

            def emit(c, value):
                dst[:, spans[c]] = value
                for h in range(E):
                    rows = slice(h * 8, h * 8 + 8)
                    base = adj[t, rows, spans[c]] if at == 0 else forc[t * E + h, :, spans[c]]
                    forc[t * E + h, :, spans[c]] = base + value[rows]
                rim = value[crow:] if at == 0 else rims[:, spans[c]] + value[crow:]
                if at < STEPS - 2:
                    rims[:, spans[c]] = rim
                else:
                    for r in range(3):
                        edge[0, t, r, :, spans[c]] = rim[r : r + 1]
                        edge[1, t, r, :, spans[c]] = rim[r + 5 : r + 6]

            back(t, src, emit)

    def send_set(t, turn_of):
        @pl.when(has_up & turn_of)
        def _():
            edge_up[t].start()

        @pl.when(has_down & turn_of)
        def _():
            edge_down[t].start()

        for h in range(E):
            here = (k == level[t]) & (e == h)

            @pl.when(here & turn_of)
            def _():
                rs_v[k] = forc[t * E + h]

            @pl.when(jnp.logical_not(here) & turn_of)
            def _():
                owner_copy(t, h).start()

    round_on(1)
    for t in range(half):
        advance(t)
        if t == half - 1:
            p_copy.start()
        if t < half // 2:
            @pl.when(has_later)
            def _():
                e_copy(t).start()

    observe()
    for t in range(half):
        @pl.when(has_later)
        def _():
            n_copy[t].wait_recv()

        retreat(t)
        if t == 0:
            round_on(2)
        send_set(t, e == 0 if near and t == half - 1 else e >= 0)

    owner = k // half == role

    def all_but(ref, some):
        return ref.at[pl.ds(0, ref.shape[0] - some)]

    def sent_all():
        for some, when in ((1, owner), (0, jnp.logical_not(owner))):
            @pl.when(when)
            def _():
                remote(all_but(forc, some), all_but(forc, some), rs_ssem, rs_rsem, partner).wait_send()

    def send_end():
        for t in range(half // 2, half):
            e_copy(t).start()

    for t in range(half):
        def emit(c, value):
            last[t, :, spans[c]] = value[0:crow]
            a_up_v[t, :, spans[c]] = value[crow : crow + 4]
            a_down_v[t, :, spans[c]] = value[crow + 4 :]

        back(t, (adj.at[t], wide.at[0, t])[STEPS % 2 == 0], emit)
    if near:
        send_set(half - 1, e != 0)

    @pl.when(has_later & (k != 1))
    def _():
        send_end()

    a_up = remote(a_up_v, a_before, a_ssem.at[0], a_rsem.at[0], up)
    a_down = remote(a_down_v, a_after, a_ssem.at[1], a_rsem.at[1], down)

    @pl.when(has_up)
    def _():
        a_up.start()

    @pl.when(has_down)
    def _():
        a_down.start()

    @pl.when(k == 1)
    def _():
        sent_all()

        @pl.when(e == 0)
        def _():
            pl.semaphore_signal(round_sem.at[1], inc=1, device_id=partner, device_id_type=MESH)

        @pl.when(e != 0)
        def _():
            pl.semaphore_wait(round_sem.at[1], 1)

        @pl.when(has_later)
        def _():
            send_end()

    p_copy.wait_recv()
    for some, when in ((1, owner), (0, jnp.logical_not(owner))):
        @pl.when(when)
        def _():
            remote(all_but(rs_v, some), all_but(rs_v, some), rs_ssem, rs_rsem, partner).wait_recv()

    @pl.when(edge_in)
    def _():
        remote(edge_v, edge_v, ed_ssem.at[0], ed_rsem, partner).wait_recv()

    total = rs_v[0]
    for at in range(1, T):
        total = total + rs_v[at]
    inner = [sum((edge_v[at, r] for at in range(1, T)), edge_v[0, r]) for r in range(3)]
    blank = jnp.zeros((5, width), jnp.float32)
    total = total + jnp.where(
        e == 0, jnp.concatenate(inner + [blank], axis=0), jnp.concatenate([blank] + inner, axis=0)
    )
    total = total[:, 0:lon]
    lane = lax.broadcasted_iota(jnp.int32, (8, 128), 1)
    part = jnp.zeros((8, 128), jnp.float32)
    for m in range(E * members):
        dots = jnp.sum(pert_v[m // members, m % members, e] * total, axis=1, keepdims=True)
        part = jnp.where(lane == m, dots, part)
    part = jnp.sum(part, axis=0, keepdims=True)
    ca_send[...] = part
    if direct:
        crowd = [(dt, lat, de) for lat in range(L) for dt in range(T) for de in range(E)]
        if not near:
            pl.semaphore_wait(all_sem, L - 1)
    else:
        crowd = [(dt, b, de) for dt, de in group]

    def seat(dt, lat, de):
        at, ens = lax.rem(k + dt, T), lax.rem(e + de, E)
        index = (at * L + lat) * E + ens if direct else at * E + ens
        return index, {"tm": at, "lat": lat, "ens": ens}

    sums = cb_v if direct else ca_v
    me, _ = seat(0, b, 0)
    sums[me] = part
    for dt, lat, de in crowd:
        copy = remote(ca_send, sums.at[me], ca_ssem, ca_rsem, seat(dt, lat, de)[1])
        if dt or de:
            copy.start()
        else:
            @pl.when(lat != b)
            def _():
                copy.start()

    @pl.when(has_prior)
    def _():
        remote(end_v, prior_v, e_ssem, e_rsem, partner).wait_recv()

    @pl.when(has_down)
    def _():
        a_up.wait_recv()

    @pl.when(has_up)
    def _():
        a_down.wait_recv()

    p_copy.wait_send()
    for t in range(half):
        prec = mp_ref[level[t]]
        gap = jnp.zeros((crow - 8, lon), jnp.float32)
        rims_in = jnp.concatenate([a_before[t][:, 0:lon], gap, a_after[t][:, 0:lon]], axis=0)
        grad_v[level[t]] = last[t, :, 0:lon] + rims_in + prec * (fields[0, t] - prior_v[t, :, 0:lon])
        remote(grad_v.at[level[t]], grad_v.at[level[t]], p_ssem, g_rsem, partner).start()
    grad_half = grad_v.at[pl.ds(0, half)]
    g_copy = remote(grad_half, grad_half, p_ssem, g_rsem, partner)
    others = all_but(sums, 1)
    remote(others, others, ca_ssem, ca_rsem, partner).wait_recv()
    if not direct:
        part = ca_v[0]
        for at in range(1, T * E):
            part = part + ca_v[at]
        cb_send[...] = part
        cb_v[b] = part
        for db in range(1, L):
            remote(cb_send, cb_v.at[b], cb_ssem, cb_rsem, {"lat": lax.rem(b + db, L)}).start()
        bands = remote(all_but(cb_v, 1), all_but(cb_v, 1), cb_ssem, cb_rsem, partner)
        bands.wait_recv()
    g_copy.wait_recv()

    @pl.when(k != 1)
    def _():
        sent_all()

    @pl.when(has_up)
    def _():
        remote(h_last, h_before, h_ssem.at[0], h_rsem.at[0, 0], up).wait_send()
        a_up.wait_send()
        remote(edge.at[0], edge.at[0], ed_ssem.at[0], ed_rsem, up).wait_send()

    @pl.when(has_down)
    def _():
        remote(h_first, h_after, h_ssem.at[1], h_rsem.at[1, 0], down).wait_send()
        a_down.wait_send()
        remote(edge.at[1], edge.at[1], ed_ssem.at[1], ed_rsem, down).wait_send()

    @pl.when(has_prior)
    def _():
        remote(nxt_v, nxt_v, t_ssem, t_rsem.at[0], partner).wait_send()

    @pl.when(has_later)
    def _():
        remote(end_v, end_v, e_ssem, e_rsem, partner).wait_send()

    g_copy.wait_send()
    remote(others, others, ca_ssem, ca_rsem, partner).wait_send()
    if not direct:
        bands.wait_send()


def finish(grad_v, pert_v, cb_v, grad_hbm, step_hbm, step_v, out_sem):
    g_out = pltpu.make_async_copy(grad_v, grad_hbm, out_sem.at[0])
    g_out.start()
    ens, members, rows, _, lon = pert_v.shape
    count = ens * members
    parts = [cb_v[at] for at in range(cb_v.shape[0])]
    while len(parts) > 1:
        parts = [sum(parts[at + 1 : at + 2], parts[at]) for at in range(0, len(parts), 2)]
    part = parts[0]
    factor = jnp.broadcast_to(part, (8, 128)) * (-1.0 / (count - 1.0))
    for h in range(rows):
        mixed = jnp.zeros((8, lon), jnp.float32)
        for m in range(count):
            mixed = mixed + factor[:, m : m + 1] * pert_v[m // members, m % members, h]
        step_v[h * 8 : h * 8 + 8, :] = mixed
    s_out = pltpu.make_async_copy(step_v, step_hbm, out_sem.at[1])
    s_out.start()
    g_out.wait()
    s_out.wait()


def on_device(T, L, E, increment, wind_lon, wind_lat, model_precision, perturbations, obs_rows, obs_jacobian,
              obs_values, obs_precision, obs_counts):
    _, levels, crow, lon = increment.shape
    members = perturbations.shape[0]
    blocks, slots = obs_jacobian.shape[1:3]
    half, width = levels // E, -(-lon // 128) * 128
    heard = T * L * E if T * L * E <= 64 else L
    f32, dma = jnp.float32, pltpu.SemaphoreType.DMA
    vmem, anyw = pl.BlockSpec(memory_space=pltpu.VMEM), pl.BlockSpec(memory_space=pl.ANY)

    def buf(*shape, kind=f32):
        return pltpu.VMEM(shape, kind)

    table = buf(blocks, slots // 8, 8, 128)
    parts = pl.pallas_call(
        functools.partial(kernel, T, L, E),
        out_shape=(
            buf(levels, crow, lon),
            buf(E, members, crow // 8, 8, lon),
            buf(heard, 1, 128),
        ),
        in_specs=[pl.BlockSpec(memory_space=pltpu.HBM)] * 10,
        out_specs=(vmem, vmem, vmem),
        scratch_shapes=[
            pltpu.SMEM((1, blocks), jnp.int32), pltpu.VMEM((2, 1, blocks), jnp.int32), buf(2, slots, blocks), pltpu.SMEM((levels,), f32),
            buf(3, half, crow, lon), buf(blocks, slots // 8, 8, lon), table, table, table, table, table,
            buf(half * crow, blocks * 8, kind=jnp.bfloat16),
            buf(3, half, 24, width), buf(half, 5, 24, width), buf(half, 24, width),
            buf(half, 5, 2, width), buf(half, 5, 2, width), buf(half, 5, 2, width), buf(half, 5, 2, width),
            buf(half, 4, width), buf(half, 4, width), buf(half, 4, width), buf(half, 4, width),
            buf(half, crow, width), buf(half, crow, 1, width), buf(half, crow, width), buf(8, width), buf(half, crow, lon), buf(half, crow, width),
            buf(half * E, 8, width), buf(2, half, 3, 1, width), buf(T, 8, width), buf(T, 3, 1, width),
            buf(1, 128), buf(T * E, 1, 128), buf(1, 128),
            dma((2,)), dma((4,)), dma((2,)), dma((2, half)), dma((2,)), dma((2,)), dma, dma((half,)), dma, dma,
            dma, dma, dma, dma, dma((2,)), dma, dma, dma, dma, dma, dma, pltpu.SemaphoreType.REGULAR,
            pltpu.SemaphoreType.REGULAR((2,)),
        ],
        compiler_params=pltpu.CompilerParams(
            collective_id=0, has_side_effects=True, vmem_limit_bytes=56 * 1024 * 1024
        ),
    )(
        obs_rows, obs_counts, obs_values[0].T, obs_precision[0].T, model_precision,
        increment[0], wind_lon[0], wind_lat[0],
        obs_jacobian.reshape(blocks, slots // 8, 8, lon),
        perturbations.reshape(members, crow // 8, 8, lon),
    )
    grad, step = pl.pallas_call(
        finish,
        out_shape=(
            jax.ShapeDtypeStruct((levels, crow, lon), f32),
            jax.ShapeDtypeStruct((crow, lon), f32),
        ),
        in_specs=[vmem] * 3,
        out_specs=(anyw, anyw),
        scratch_shapes=[buf(crow, lon), dma((2,))],
        compiler_params=pltpu.CompilerParams(vmem_limit_bytes=8 * 1024 * 1024),
    )(*[pltpu.with_memory_space_constraint(item, pltpu.VMEM) for item in parts])
    return grad[None], step[None]


def solution(mesh):
    T, L, E = mesh.shape["tm"], mesh.shape["lat"], mesh.shape["ens"]
    placed = (
        P("tm", None, "lat", None),
        P("tm", None, "lat", None),
        P("tm", None, "lat", None),
        P(),
        P("ens", "tm", "lat", None),
        P("tm", "lat"),
        P("tm", "lat", None, None),
        P("tm", "lat", None),
        P("tm", "lat", None),
        P("tm", "lat"),
    )
    return jax.shard_map(
        functools.partial(on_device, T, L, E),
        mesh=mesh,
        in_specs=placed,
        out_specs=(P("tm", None, "lat", None), P("tm", "lat", None)),
        check_vma=False,
    )
```

```python
import functools

import jax
import jax.numpy as jnp
from jax import lax
from jax.experimental import pallas as pl
from jax.experimental.pallas import tpu as pltpu
from jax.sharding import PartitionSpec as P

STEPS = 4
MESH = pl.DeviceIdType.MESH
HIGHEST = lax.Precision.HIGHEST
NN = (((1,), (0,)), ((), ()))


def mm(a, b, dims, precision=None):
    return lax.dot_general(a, b, dims, precision=precision, preferred_element_type=jnp.float32)


def split(value):
    hi = value.astype(jnp.bfloat16)
    lo = (value - hi.astype(jnp.float32)).astype(jnp.bfloat16)
    return hi, lo


def turn(value, steps, axis):
    return pltpu.roll(value, steps % value.shape[axis], axis)


def extend(ref, where, lon):
    width = ref.shape[-1]
    rem = lon % 128
    last = ref[where + (slice(0, 16), slice(width - 128, width))]
    before = ref[where + (slice(0, 16), slice(width - 256, width - 128))]
    first = ref[where + (slice(0, 16), slice(0, 128))]
    lane = lax.broadcasted_iota(jnp.int32, last.shape, 1)
    wrapped = jnp.where(lane < 128 - rem, turn(before, 128 - rem, 1), turn(last, 128 - rem, 1))
    right = jnp.where(lane < rem + (128 - rem) // 2, turn(first, rem, 1), wrapped)
    ref[where + (slice(0, 16), slice(width - 128, width))] = jnp.where(lane < rem, last, right)


def kernel(
    T, L, E,
    rows_hbm, cnt_hbm, val_hbm, prc_hbm, mp_hbm, inc_hbm, wlon_hbm, wlat_hbm, jac_hbm, pert_hbm,
    grad_v, pert_v, cb_v,
    rows_s, whole_ref, slot_ref, mp_ref, fields, jac_v, tail, val_b, prc_b, part_v, wgt, pick,
    wide, coef, adj, h_first, h_last, h_after, h_before, a_up_v, a_down_v, a_after, a_before,
    end_v, lines, last, rims, nxt_v, prior_v, forc, edge, rs_v, edge_v, ca_send, ca_v, cb_send,
    load_sem, small_sem, h_ssem, h_rsem, a_ssem, a_rsem, t_ssem, t_rsem, e_ssem, e_rsem, p_ssem, p_rsem,
    rs_ssem, rs_rsem, ed_ssem, ed_rsem, sum_sem, g_rsem, round_sem,
):
    k, b, e = lax.axis_index("tm"), lax.axis_index("lat"), lax.axis_index("ens")
    _, half, crow, lon = fields.shape
    width = wide.shape[-1]
    members = pert_v.shape[1]
    _, slots, blocks = slot_ref.shape
    tiles, rem = width // 128, lon % 128
    other = 1 - e

    direct = T * L * E <= 64
    near = direct and T == 4 and E == 2
    role = lax.rem(e + k // 2, 2) if near else e

    def shift(at, core):
        return lax.rem(at + 1 + core, half)

    def keeper(at):
        return lax.rem(e + k // 2 + at // 2, 2) if near else e

    def spot(t, at, core, there, other_core):
        return lax.rem(t + shift(at, core) + half - shift(there, other_core), half)

    order = [lax.rem(shift(k, e) + t, half) for t in range(half)]
    level = [role * half + at for at in order]

    ca_ssem, ca_rsem = sum_sem.at[0], sum_sem.at[1]

    def local(src, dst, sem):
        return pltpu.make_async_copy(src, dst, sem)

    for at, ref in enumerate((inc_hbm, wlon_hbm, wlat_hbm)):
        for t in range(half):
            local(ref.at[level[t]], fields.at[at, t], load_sem.at[0]).start()
    small = [
        local(rows_hbm, rows_s, small_sem.at[0]),
        local(rows_hbm, whole_ref.at[0], small_sem.at[1]),
        local(cnt_hbm, whole_ref.at[1], small_sem.at[1]),
        local(val_hbm, slot_ref.at[0], small_sem.at[2]),
        local(prc_hbm, slot_ref.at[1], small_sem.at[2]),
        local(mp_hbm, mp_ref, small_sem.at[3]),
    ]

    barrier = pltpu.get_barrier_semaphore()
    group = [(dt, de) for dt in range(T) for de in range(E) if dt or de]

    def mate(dt, de):
        return {"tm": lax.rem(k + dt, T), "ens": lax.rem(e + de, E)}

    ring = [
        ({"ens": 1 - e}, None),
        ({"tm": k + 1 - 2 * lax.rem(k, 2)}, None),
        ({"tm": lax.rem(k + 2, T)}, None),
        ({"lat": lax.rem(b + 1, L)}, b < L - 1),
        ({"lat": lax.rem(b + L - 1, L)}, b > 0),
    ]
    middle = (k == 1) | (k == 2)

    def greet(sem, extra):
        for device, when in ring + ([({"tm": T - 1 - k, "ens": other}, middle)] if extra else []):
            if when is None:
                pl.semaphore_signal(sem, inc=1, device_id=device, device_id_type=MESH)
            else:
                @pl.when(when)
                def _():
                    pl.semaphore_signal(sem, inc=1, device_id=device, device_id_type=MESH)

    def meet(sem, extra):
        count = 3 + (b < L - 1).astype(jnp.int32) + (b > 0).astype(jnp.int32)
        pl.semaphore_wait(sem, count + middle.astype(jnp.int32) if extra else count)

    def round_on(at):
        if near:
            meet(round_sem.at[at % 2], False)
            if at < 2:
                greet(round_sem.at[(at + 1) % 2], False)

    if near:
        greet(barrier, True)
    else:
        for dt, de in group:
            pl.semaphore_signal(barrier, inc=1, device_id=mate(dt, de), device_id_type=MESH)
        for db in range(1, L):
            pl.semaphore_signal(barrier, inc=1, device_id={"lat": lax.rem(b + db, L)}, device_id_type=MESH)

    def remote(src, dst, ssem, rsem, device):
        return pltpu.make_async_remote_copy(
            src_ref=src, dst_ref=dst, send_sem=ssem, recv_sem=rsem, device_id=device, device_id_type=MESH
        )

    up = {"lat": lax.rem(b + 1, L)}
    down = {"lat": lax.rem(b + L - 1, L)}
    later_k, prior_k = lax.rem(k + 1, T), lax.rem(k + T - 1, T)
    partner = {"ens": other}
    has_up, has_down = b < L - 1, b > 0
    has_later, has_prior = k < T - 1, k > 0

    local(fields, fields, load_sem.at[0]).wait()
    jac_load = local(jac_hbm, jac_v, load_sem.at[0])
    pert_load = local(pert_hbm, pert_v.at[e], load_sem.at[1])
    for item in small + [pert_load, jac_load]:
        item.start()
    for t in range(half):
        for at in range(3):
            wide[at, t, 0:16, 0:lon] = fields[at, t]
            extend(wide, (at, t), lon)
        h_first[t, 0] = wide[0, t, 0:2]
        h_first[t, 1] = wide[0, t, 2:4]
        h_last[t, 0] = wide[0, t, crow - 4 : crow - 2]
        h_last[t, 1] = wide[0, t, crow - 2 : crow]
        for at in (1, 2):
            h_first[t, 1 + at] = wide[at, t, 0:2]
            h_first[t, 4, at - 1 : at] = wide[at, t, 2:3]
            h_last[t, 1 + at] = wide[at, t, crow - 2 : crow]
            h_last[t, 4, at - 1 : at] = wide[at, t, crow - 3 : crow - 2]

    if near:
        meet(barrier, True)
    else:
        pl.semaphore_wait(barrier, len(group) + L - 1)
        if direct:
            for db in range(1, L):
                pl.semaphore_signal(round_sem.at[0], inc=1, device_id={"lat": lax.rem(b + db, L)}, device_id_type=MESH)

    h_up = [remote(h_last.at[t], h_before.at[t], h_ssem.at[0], h_rsem.at[0, t], up) for t in range(half)]
    h_down = [remote(h_first.at[t], h_after.at[t], h_ssem.at[1], h_rsem.at[1, t], down) for t in range(half)]
    n_copy = [
        remote(fields.at[0, spot(t, prior_k, keeper(prior_k), k, e)], nxt_v.at[t], t_ssem, t_rsem.at[t], {"tm": prior_k, "ens": keeper(prior_k)})
        for t in range(half)
    ]

    def e_copy(t):
        there = spot(t, k, e, later_k, keeper(later_k))
        return remote(end_v.at[t], prior_v.at[there], e_ssem, e_rsem, {"tm": later_k, "ens": keeper(later_k)})

    for t in range(half):
        @pl.when(has_up)
        def _():
            h_up[t].start()

        @pl.when(has_down)
        def _():
            h_down[t].start()

    for t in range(half):
        @pl.when(has_prior)
        def _():
            n_copy[t].start()

    if near:
        greet(round_sem.at[0], False)
    pert_load.wait()
    p_copy = remote(pert_v.at[e], pert_v.at[e], p_ssem, p_rsem, partner)

    @pl.when(jnp.logical_not(has_up))
    def _():
        h_after[...] = jnp.zeros_like(h_after)
        a_after[...] = jnp.zeros_like(a_after)

    @pl.when(jnp.logical_not(has_down))
    def _():
        h_before[...] = jnp.zeros_like(h_before)
        a_before[...] = jnp.zeros_like(a_before)

    @pl.when(jnp.logical_not(has_prior))
    def _():
        prior_v[...] = jnp.zeros_like(prior_v)

    @pl.when(jnp.logical_not(has_later))
    def _():
        nxt_v[...] = jnp.zeros_like(nxt_v)

    edge_in = ((e == 0) & has_down) | ((e == E - 1) & has_up)

    @pl.when(jnp.logical_not(edge_in))
    def _():
        edge_v[...] = jnp.zeros_like(edge_v)

    def weigh(t, rows):
        wl, wt = wide[1, t, rows], wide[2, t, rows]
        wl2, wt2 = wl * wl, wt * wt
        coef[t, 0, rows] = 1.0 - wl2 - wt2
        coef[t, 1, rows] = 0.5 * (wl2 - wl)
        coef[t, 2, rows] = 0.5 * (wl2 + wl)
        coef[t, 3, rows] = 0.5 * (wt2 - wt)
        coef[t, 4, rows] = 0.5 * (wt2 + wt)

    for t in range(half):
        weigh(t, slice(0, crow))
        for at in (1, 2):
            wide[at, t, crow : crow + 8] = jnp.zeros((8, width), jnp.float32)

    for item in (
        small[0], small[-1], local(whole_ref, whole_ref, small_sem.at[1]), local(slot_ref, slot_ref, small_sem.at[2])
    ):
        item.wait()
    deep = lax.broadcasted_iota(jnp.int32, (slots, blocks), 0)
    precisions = jnp.where(deep < whole_ref[1], slot_ref[1], 0.0)
    values = slot_ref[0]
    for j in range(blocks):
        prc_b[j] = jnp.broadcast_to(precisions[:, j : j + 1], (slots, 128)).reshape(slots // 8, 8, 128)
        val_b[j] = jnp.broadcast_to(values[:, j : j + 1], (slots, 128)).reshape(slots // 8, 8, 128)
    column = lax.broadcasted_iota(jnp.int32, (blocks, blocks * 8), 1)
    block = lax.broadcasted_iota(jnp.int32, (blocks, blocks * 8), 0)
    spread = ((column >= block * 8) & (column < (block + 1) * 8)).astype(jnp.float32)
    rows = mm(jnp.broadcast_to(whole_ref[0].astype(jnp.float32), (8, blocks)), spread, NN, HIGHEST)[0:1]
    line = lax.broadcasted_iota(jnp.int32, (crow, blocks * 8), 0)
    for t in range(half):
        wanted = (line + level[t] * crow).astype(jnp.float32)
        pick[t * crow : (t + 1) * crow] = (jnp.abs(rows - wanted) < 0.5).astype(jnp.bfloat16)

    round_on(0)
    jac_load.wait()
    if rem:
        tail[...] = jnp.zeros_like(tail)
        tail[:, :, :, 0:rem] = jac_v[:, :, :, lon - rem : lon]

    def strip(at, c):
        if rem and c == tiles - 1:
            return tail[at]
        return jac_v[at, :, :, c * 128 : (c + 1) * 128]

    def observe():
        def measure(base, carry):
            for u in range(16):
                j = base * 16 + u
                row = rows_s[0, j]
                slot = lax.rem(row // crow + half - shift(k, e), half)
                row = lax.rem(row, crow)
                total = strip(j, 0) * lines[slot, row, :, spans[0]]
                for c in range(1, tiles):
                    total = total + strip(j, c) * lines[slot, row, :, spans[c]]
                part_v[j] = total
            return carry

        lax.fori_loop(0, blocks // 16, measure, 0)
        evolved = jnp.sum(part_v[...], axis=-1, keepdims=True)
        wgt[...] = prc_b[...] * (evolved - val_b[...])
        for c in range(0, tiles, 2):
            pieces = []
            for cc in range(c, min(c + 2, tiles)):
                piece = jnp.sum(strip(slice(None), cc) * wgt[...], axis=1)
                pieces.append(piece.reshape(blocks * 8, 128))
            hi, lo = split(jnp.concatenate(pieces, axis=1))
            placed = mm(pick[...], hi, NN) + mm(pick[...], lo, NN)
            for t in range(half):
                adj[t, 0:crow, c * 128 : c * 128 + hi.shape[1]] = placed[t * crow : (t + 1) * crow]

    lane = lax.broadcasted_iota(jnp.int32, (24, 128), 1)
    starts, stops = lane == 0, lane == 127
    spans = [slice(c * 128, (c + 1) * 128) for c in range(tiles)]

    def forward(t, src, emit):
        east = turn(src[:, spans[-1]], 1, 1)
        here = src[:, spans[0]]
        west = first_west = turn(here, -1, 1)
        for c in range(tiles):
            f, f_west, f_east = here, west, turn(here, 1, 1)
            if c + 1 < tiles:
                here = src[:, spans[c + 1]]
                west = turn(here, -1, 1)
            after = west if c + 1 < tiles else first_west
            emit(c, (
                coef[t, 0, :, spans[c]] * f
                + coef[t, 1, :, spans[c]] * jnp.where(stops, after, f_west)
                + coef[t, 2, :, spans[c]] * jnp.where(starts, east, f_east)
                + coef[t, 3, :, spans[c]] * turn(f, -1, 0)
                + coef[t, 4, :, spans[c]] * turn(f, 1, 0)
            ))
            east = f_east

    def back(t, src, emit):
        def moved(c):
            g = src[:, spans[c]]
            return g, turn(coef[t, 1, :, spans[c]] * g, 1, 1), turn(coef[t, 2, :, spans[c]] * g, -1, 1)

        east = moved(tiles - 1)[1]
        now = first = moved(0)
        for c in range(tiles):
            g, g_east, g_west = now
            if c + 1 < tiles:
                now = moved(c + 1)
            after = now[2] if c + 1 < tiles else first[2]
            emit(c, (
                coef[t, 0, :, spans[c]] * g
                + jnp.where(starts, east, g_east)
                + jnp.where(stops, after, g_west)
                + turn(coef[t, 3, :, spans[c]] * g, 1, 0)
                + turn(coef[t, 4, :, spans[c]] * g, -1, 0)
            ))
            east = g_east

    def owner_copy(t, h):
        return remote(forc.at[t * E + h], rs_v.at[k], rs_ssem, rs_rsem, {"tm": level[t], "ens": h})

    def edge_copy(t, h, device):
        return remote(edge.at[h, t], edge_v.at[k], ed_ssem.at[h], ed_rsem, device)

    edge_up = [edge_copy(t, 0, {"tm": level[t], "lat": lax.rem(b + 1, L), "ens": 0}) for t in range(half)]
    edge_down = [edge_copy(t, 1, {"tm": level[t], "lat": lax.rem(b + L - 1, L), "ens": E - 1}) for t in range(half)]

    pairs = [(wide.at[0, t], adj.at[t]) for t in range(half)]

    def advance(t):
        @pl.when(has_down)
        def _():
            h_up[t].wait_recv()

        @pl.when(has_up)
        def _():
            h_down[t].wait_recv()

        wide[0, t, crow : crow + 2] = h_after[t, 0]
        wide[0, t, crow + 2 : crow + 4] = h_after[t, 1]
        wide[0, t, crow + 4 : crow + 6] = h_before[t, 0]
        wide[0, t, crow + 6 : crow + 8] = h_before[t, 1]
        for at in (1, 2):
            wide[at, t, crow : crow + 2] = h_after[t, 1 + at]
            wide[at, t, crow + 2 : crow + 3] = h_after[t, 4, at - 1 : at]
            wide[at, t, crow + 5 : crow + 6] = h_before[t, 4, at - 1 : at]
            wide[at, t, crow + 6 : crow + 8] = h_before[t, 1 + at]
        weigh(t, slice(crow, crow + 8))
        for at in range(STEPS):
            src, dst = pairs[t][at % 2], pairs[t][(at + 1) % 2]

            def emit(c, value):
                if at + 1 < STEPS:
                    dst[:, spans[c]] = value
                else:
                    end_v[t, :, spans[c]] = value[0:crow]
                    for r in range(crow):
                        lines[t, r, :, spans[c]] = value[r : r + 1]

            forward(t, src, emit)

    def retreat(t):
        scale = jnp.where(has_later, mp_ref[level[t]], 0.0)
        adj[t, 0:crow, 0:lon] = adj[t, 0:crow, 0:lon] - scale * (nxt_v[t] - end_v[t, :, 0:lon])
        extend(adj, (t,), lon)
        adj[t, crow : crow + 8] = jnp.zeros((8, width), jnp.float32)
        for at in range(STEPS - 1):
            src, dst = pairs[t][(at + 1) % 2], pairs[t][at % 2]

            def emit(c, value):
                dst[:, spans[c]] = value
                for h in range(E):
                    rows = slice(h * 8, h * 8 + 8)
                    base = adj[t, rows, spans[c]] if at == 0 else forc[t * E + h, :, spans[c]]
                    forc[t * E + h, :, spans[c]] = base + value[rows]
                rim = value[crow:] if at == 0 else rims[:, spans[c]] + value[crow:]
                if at < STEPS - 2:
                    rims[:, spans[c]] = rim
                else:
                    for r in range(3):
                        edge[0, t, r, :, spans[c]] = rim[r : r + 1]
                        edge[1, t, r, :, spans[c]] = rim[r + 5 : r + 6]

            back(t, src, emit)

    def send_set(t, turn_of):
        @pl.when(has_up & turn_of)
        def _():
            edge_up[t].start()

        @pl.when(has_down & turn_of)
        def _():
            edge_down[t].start()

        for h in range(E):
            here = (k == level[t]) & (e == h)

            @pl.when(here & turn_of)
            def _():
                rs_v[k] = forc[t * E + h]

            @pl.when(jnp.logical_not(here) & turn_of)
            def _():
                owner_copy(t, h).start()

    round_on(1)
    for t in range(half):
        advance(t)
        if t == half - 1:
            p_copy.start()
        if t < half // 2:
            @pl.when(has_later)
            def _():
                e_copy(t).start()

    observe()
    for t in range(half):
        @pl.when(has_later)
        def _():
            n_copy[t].wait_recv()

        retreat(t)
        if t == 0:
            round_on(2)
        send_set(t, e == 0 if near and t == half - 1 else e >= 0)

    owner = k // half == role

    def all_but(ref, some):
        return ref.at[pl.ds(0, ref.shape[0] - some)]

    def sent_all():
        for some, when in ((1, owner), (0, jnp.logical_not(owner))):
            @pl.when(when)
            def _():
                remote(all_but(forc, some), all_but(forc, some), rs_ssem, rs_rsem, partner).wait_send()

    def send_end():
        for t in range(half // 2, half):
            e_copy(t).start()

    for t in range(half):
        def emit(c, value):
            last[t, :, spans[c]] = value[0:crow]
            a_up_v[t, :, spans[c]] = value[crow : crow + 4]
            a_down_v[t, :, spans[c]] = value[crow + 4 :]

        back(t, (adj.at[t], wide.at[0, t])[STEPS % 2 == 0], emit)
    if near:
        send_set(half - 1, e != 0)

    @pl.when(has_later & (k != 1))
    def _():
        send_end()

    a_up = remote(a_up_v, a_before, a_ssem.at[0], a_rsem.at[0], up)
    a_down = remote(a_down_v, a_after, a_ssem.at[1], a_rsem.at[1], down)

    @pl.when(has_up)
    def _():
        a_up.start()

    @pl.when(has_down)
    def _():
        a_down.start()

    @pl.when(k == 1)
    def _():
        sent_all()

        @pl.when(e == 0)
        def _():
            pl.semaphore_signal(round_sem.at[1], inc=1, device_id=partner, device_id_type=MESH)

        @pl.when(e != 0)
        def _():
            pl.semaphore_wait(round_sem.at[1], 1)

        @pl.when(has_later)
        def _():
            send_end()

    p_copy.wait_recv()
    for some, when in ((1, owner), (0, jnp.logical_not(owner))):
        @pl.when(when)
        def _():
            remote(all_but(rs_v, some), all_but(rs_v, some), rs_ssem, rs_rsem, partner).wait_recv()

    @pl.when(edge_in)
    def _():
        remote(edge_v, edge_v, ed_ssem.at[0], ed_rsem, partner).wait_recv()

    total = rs_v[0]
    for at in range(1, T):
        total = total + rs_v[at]
    inner = [sum((edge_v[at, r] for at in range(1, T)), edge_v[0, r]) for r in range(3)]
    blank = jnp.zeros((5, width), jnp.float32)
    total = total + jnp.where(
        e == 0, jnp.concatenate(inner + [blank], axis=0), jnp.concatenate([blank] + inner, axis=0)
    )
    total = total[:, 0:lon]
    lane = lax.broadcasted_iota(jnp.int32, (8, 128), 1)
    part = jnp.zeros((8, 128), jnp.float32)
    for m in range(E * members):
        dots = jnp.sum(pert_v[m // members, m % members, e] * total, axis=1, keepdims=True)
        part = jnp.where(lane == m, dots, part)
    part = jnp.sum(part, axis=0, keepdims=True)
    ca_send[...] = part
    if direct:
        crowd = [(dt, lat, de) for lat in range(L) for dt in range(T) for de in range(E)]
        if not near:
            pl.semaphore_wait(round_sem.at[0], L - 1)
    else:
        crowd = [(dt, b, de) for dt, de in group]

    def seat(dt, lat, de):
        at, ens = lax.rem(k + dt, T), lax.rem(e + de, E)
        index = (at * L + lat) * E + ens if direct else at * E + ens
        return index, {"tm": at, "lat": lat, "ens": ens}

    sums = cb_v if direct else ca_v
    me, _ = seat(0, b, 0)
    sums[me] = part
    for dt, lat, de in crowd:
        copy = remote(ca_send, sums.at[me], ca_ssem, ca_rsem, seat(dt, lat, de)[1])
        if dt or de:
            copy.start()
        else:
            @pl.when(lat != b)
            def _():
                copy.start()

    @pl.when(has_prior)
    def _():
        remote(end_v, prior_v, e_ssem, e_rsem, partner).wait_recv()

    @pl.when(has_down)
    def _():
        a_up.wait_recv()

    @pl.when(has_up)
    def _():
        a_down.wait_recv()

    p_copy.wait_send()
    for t in range(half):
        prec = mp_ref[level[t]]
        gap = jnp.zeros((crow - 8, lon), jnp.float32)
        rims_in = jnp.concatenate([a_before[t][:, 0:lon], gap, a_after[t][:, 0:lon]], axis=0)
        grad_v[level[t]] = last[t, :, 0:lon] + rims_in + prec * (fields[0, t] - prior_v[t, :, 0:lon])
        remote(grad_v.at[level[t]], grad_v.at[level[t]], p_ssem, g_rsem, partner).start()
    grad_half = grad_v.at[pl.ds(0, half)]
    g_copy = remote(grad_half, grad_half, p_ssem, g_rsem, partner)
    others = all_but(sums, 1)
    remote(others, others, ca_ssem, ca_rsem, partner).wait_recv()
    if not direct:
        part = ca_v[0]
        for at in range(1, T * E):
            part = part + ca_v[at]
        cb_ssem, cb_rsem = sum_sem.at[2], sum_sem.at[3]
        cb_send[...] = part
        cb_v[b] = part
        for db in range(1, L):
            remote(cb_send, cb_v.at[b], cb_ssem, cb_rsem, {"lat": lax.rem(b + db, L)}).start()
        bands = remote(all_but(cb_v, 1), all_but(cb_v, 1), cb_ssem, cb_rsem, partner)
        bands.wait_recv()
    g_copy.wait_recv()

    @pl.when(k != 1)
    def _():
        sent_all()

    @pl.when(has_up)
    def _():
        remote(h_last, h_before, h_ssem.at[0], h_rsem.at[0, 0], up).wait_send()
        a_up.wait_send()
        remote(edge.at[0], edge.at[0], ed_ssem.at[0], ed_rsem, up).wait_send()

    @pl.when(has_down)
    def _():
        remote(h_first, h_after, h_ssem.at[1], h_rsem.at[1, 0], down).wait_send()
        a_down.wait_send()
        remote(edge.at[1], edge.at[1], ed_ssem.at[1], ed_rsem, down).wait_send()

    @pl.when(has_prior)
    def _():
        remote(nxt_v, nxt_v, t_ssem, t_rsem.at[0], partner).wait_send()

    @pl.when(has_later)
    def _():
        remote(end_v, end_v, e_ssem, e_rsem, partner).wait_send()

    g_copy.wait_send()
    remote(others, others, ca_ssem, ca_rsem, partner).wait_send()
    if not direct:
        bands.wait_send()


def finish(grad_v, pert_v, cb_v, grad_hbm, step_hbm, step_v, out_sem):
    g_out = pltpu.make_async_copy(grad_v, grad_hbm, out_sem.at[0])
    g_out.start()
    ens, members, rows, _, lon = pert_v.shape
    count = ens * members
    parts = [cb_v[at] for at in range(cb_v.shape[0])]
    while len(parts) > 1:
        parts = [sum(parts[at + 1 : at + 2], parts[at]) for at in range(0, len(parts), 2)]
    part = parts[0]
    factor = jnp.broadcast_to(part, (8, 128)) * (-1.0 / (count - 1.0))
    for h in range(rows):
        mixed = jnp.zeros((8, lon), jnp.float32)
        for m in range(count):
            mixed = mixed + factor[:, m : m + 1] * pert_v[m // members, m % members, h]
        step_v[h * 8 : h * 8 + 8, :] = mixed
    s_out = pltpu.make_async_copy(step_v, step_hbm, out_sem.at[1])
    s_out.start()
    g_out.wait()
    s_out.wait()


def on_device(T, L, E, increment, wind_lon, wind_lat, model_precision, perturbations, obs_rows, obs_jacobian,
              obs_values, obs_precision, obs_counts):
    _, levels, crow, lon = increment.shape
    members = perturbations.shape[0]
    blocks, slots = obs_jacobian.shape[1:3]
    half, width = levels // E, -(-lon // 128) * 128
    heard = T * L * E if T * L * E <= 64 else L
    f32, dma = jnp.float32, pltpu.SemaphoreType.DMA
    vmem, anyw = pl.BlockSpec(memory_space=pltpu.VMEM), pl.BlockSpec(memory_space=pl.ANY)

    def buf(*shape, kind=f32):
        return pltpu.VMEM(shape, kind)

    table = buf(blocks, slots // 8, 8, 128)
    parts = pl.pallas_call(
        functools.partial(kernel, T, L, E),
        out_shape=(
            buf(levels, crow, lon),
            buf(E, members, crow // 8, 8, lon),
            buf(heard, 1, 128),
        ),
        in_specs=[pl.BlockSpec(memory_space=pltpu.HBM)] * 10,
        out_specs=(vmem, vmem, vmem),
        scratch_shapes=[
            pltpu.SMEM((1, blocks), jnp.int32), pltpu.VMEM((2, 1, blocks), jnp.int32), buf(2, slots, blocks), pltpu.SMEM((levels,), f32),
            buf(3, half, crow, lon), buf(blocks, slots // 8, 8, lon), table, table, table, table, table,
            buf(half * crow, blocks * 8, kind=jnp.bfloat16),
            buf(3, half, 24, width), buf(half, 5, 24, width), buf(half, 24, width),
            buf(half, 5, 2, width), buf(half, 5, 2, width), buf(half, 5, 2, width), buf(half, 5, 2, width),
            buf(half, 4, width), buf(half, 4, width), buf(half, 4, width), buf(half, 4, width),
            buf(half, crow, width), buf(half, crow, 1, width), buf(half, crow, width), buf(8, width), buf(half, crow, lon), buf(half, crow, width),
            buf(half * E, 8, width), buf(2, half, 3, 1, width), buf(T, 8, width), buf(T, 3, 1, width),
            buf(1, 128), buf(T * E, 1, 128), buf(1, 128),
            dma((2,)), dma((4,)), dma((2,)), dma((2, half)), dma((2,)), dma((2,)), dma, dma((half,)), dma, dma,
            dma, dma, dma, dma, dma((2,)), dma, dma((2 if T * L * E <= 64 else 4,)), dma,
            pltpu.SemaphoreType.REGULAR((2,)),
        ],
        compiler_params=pltpu.CompilerParams(
            collective_id=0, has_side_effects=True, vmem_limit_bytes=56 * 1024 * 1024
        ),
    )(
        obs_rows, obs_counts, obs_values[0].T, obs_precision[0].T, model_precision,
        increment[0], wind_lon[0], wind_lat[0],
        obs_jacobian.reshape(blocks, slots // 8, 8, lon),
        perturbations.reshape(members, crow // 8, 8, lon),
    )
    grad, step = pl.pallas_call(
        finish,
        out_shape=(
            jax.ShapeDtypeStruct((levels, crow, lon), f32),
            jax.ShapeDtypeStruct((crow, lon), f32),
        ),
        in_specs=[vmem] * 3,
        out_specs=(anyw, anyw),
        scratch_shapes=[buf(crow, lon), dma((2,))],
        compiler_params=pltpu.CompilerParams(vmem_limit_bytes=8 * 1024 * 1024),
    )(*[pltpu.with_memory_space_constraint(item, pltpu.VMEM) for item in parts])
    return grad[None], step[None]


def solution(mesh):
    T, L, E = mesh.shape["tm"], mesh.shape["lat"], mesh.shape["ens"]
    placed = (
        P("tm", None, "lat", None),
        P("tm", None, "lat", None),
        P("tm", None, "lat", None),
        P(),
        P("ens", "tm", "lat", None),
        P("tm", "lat"),
        P("tm", "lat", None, None),
        P("tm", "lat", None),
        P("tm", "lat", None),
        P("tm", "lat"),
    )
    return jax.shard_map(
        functools.partial(on_device, T, L, E),
        mesh=mesh,
        in_specs=placed,
        out_specs=(P("tm", None, "lat", None), P("tm", "lat", None)),
        check_vma=False,
    )
```
